256 devices in a mesh: branch: 4 (over x, y), seq: 64 (over z, core).
Axes of the slice: x: 2, y: 2, z: 32, core: 2. Of those that a mesh axis runs over, the one named last changes fastest.
The devices are a block of a 4x8x32 slice.
Arguments:
- queries: bfloat16 [65536, 2048], P(('branch', 'seq')), parts along dimension 0, may hold values from -8 to 8
- keys: bfloat16 [65536, 2048], P(('branch', 'seq')), parts along dimension 0, may hold values from -8 to 8
- values: bfloat16 [65536, 2048], P(('branch', 'seq')), parts along dimension 0, may hold values from -6 to 6
- out_grad: bfloat16 [65536, 2048], P(('branch', 'seq')), parts along dimension 0, may hold values from -6 to 6
- segments: int32 [65536], P(('branch', 'seq')), parts along dimension 0, may hold values from 0 to 28, never falling along the last dimension, each value on 1 to 768 neighbouring positions
Outputs:
- attended: bfloat16 [65536, 2048], P(('branch', 'seq')), parts along dimension 0
- query_grad: bfloat16 [65536, 2048], P(('branch', 'seq')), parts along dimension 0
- key_grad: bfloat16 [65536, 2048], P(('branch', 'seq')), parts along dimension 0
- value_grad: bfloat16 [65536, 2048], P(('branch', 'seq')), parts along dimension 0
The draws below stay inside these ranges and needn't reach their ends.
There are 4 independent parts, one for each index of `branch`. The reference program is written for one: setup_inputs(seed, part) draws one part's arguments, and reference() takes and returns one part's arrays. A program takes and returns all parts, laid end to end along the dimension named above; each array names one. Nothing has to cross between parts.
Inputs may be any that keep to these rules, and one draw needn't show every extreme that they name: `segments`: never falling along the sequence; each document has 1 to 768 tokens, and one has exactly 768.
All inputs are finite; a program needn't handle non-finite values.
Results may differ from the reference program's by a relative error of at most 0.017.
Values may be sent and summed in bfloat16 or wider, within the bound.
A program may use at most 128 MiB of HBM per device.

```python
import math
import jax
import jax.numpy as jnp
import numpy as np
from jax import lax

HEADS = 16
HDIM = 128
TOK_DEV = 256
REACH = 3
DOC_MAX = 768
TOKENS = 16384
DOCS = 29


def draw_queries(key, part):
    noise_key = jax.random.fold_in(key, 11)
    noise = jax.random.truncated_normal(noise_key, -6.0, 6.0, (TOKENS, HEADS * HDIM), jnp.float32)
    return noise.astype(jnp.bfloat16)


def draw_keys(key, part):
    noise_key = jax.random.fold_in(key, 13)
    noise = jax.random.truncated_normal(noise_key, -6.0, 6.0, (TOKENS, HEADS * HDIM), jnp.float32)
    return noise.astype(jnp.bfloat16)


def steps_of(rng, extent, cuts, smallest, high):
    def one(dim, blocks):
        heights = jax.random.uniform(jax.random.fold_in(jax.random.fold_in(rng, 6), dim), (blocks,), jnp.float32, smallest / len(cuts), high / len(cuts))
        return jnp.repeat(jnp.exp(heights), extent[dim] // blocks).reshape((-1,) + (1,) * (len(extent) - dim - 1))

    factor_of = one(*cuts[0])
    for cut in cuts[1:]:
        factor_of = factor_of * one(*cut)
    return factor_of


def length_profile(amount, total, most, skew):
    weights = [(1 << 20) // math.isqrt(standing ** skew) + 1 for standing in range(2, amount + 1)]
    rest, holding = total - most - (amount - 1), [1] * (amount - 1)
    while rest > 0:
        candidates = [i for i in range(amount - 1) if holding[i] < most]
        mass, budget = sum([weights[i] for i in candidates]), rest
        for i in candidates:
            addition = min(most - holding[i], max(1, budget * weights[i] // mass), rest)
            holding[i] = holding[i] + addition
            rest = rest - addition
    return np.array([most] + holding)


def ragged_sizes(own_key, count, total, reach, slope):
    if count == 2:
        one = jax.random.randint(own_key, (), max(1, total - reach), min(reach, total - 1) + 1)
        return jnp.stack([one, total - one])
    lengths = jnp.asarray(length_profile(count, total, reach, slope), jnp.int32)
    pairs = (count - 1) // 2
    donor, sink = lengths[1:1 + 2 * pairs:2], lengths[2:2 + 2 * pairs:2]
    margin = jnp.minimum(donor - 1, reach - sink)
    moved = jax.random.randint(jax.random.fold_in(own_key, 1), (pairs,), 0, 1 << 20) % (margin + 1)
    lengths = lengths.at[1:1 + 2 * pairs:2].set(donor - moved).at[2:2 + 2 * pairs:2].set(sink + moved)
    return lengths[jax.random.permutation(jax.random.fold_in(own_key, 2), count)]


def bell_draw(stream_key, dims, deviation, most, shards=(), kind=jnp.bfloat16):
    values = jax.random.normal(stream_key, dims, jnp.float32) * deviation
    if len(shards) > 0:
        values = steps_of(stream_key, dims, shards, -0.22, 0.18) * values
    return jnp.clip(values, min=-most, max=most).astype(kind)


def setup_inputs(seed: int = 0, part: int = 0) -> dict:
    arg_keys = jax.random.split(jax.random.key(seed), 6)
    part_keys = jax.random.split(jax.random.fold_in(arg_keys[5], part), 6)
    return {
        "queries": draw_queries(jax.random.fold_in(jax.random.fold_in(arg_keys[5], part), 71), part),
        "keys": draw_keys(jax.random.fold_in(jax.random.fold_in(arg_keys[5], part), 71), part),
        "values": bell_draw(part_keys[2], (TOKENS, HEADS * HDIM), 1.0, 6.0, ((0, 64),)),
        "out_grad": bell_draw(part_keys[3], (TOKENS, HEADS * HDIM), 1.0, 6.0, ((0, 64),)),
        "segments": jnp.searchsorted(jnp.cumsum(ragged_sizes(part_keys[4], DOCS, TOKENS, DOC_MAX, 1)), jnp.arange(TOKENS), side="right").astype(jnp.int32),
    }


def to_half(tensor):
    return lax.optimization_barrier(tensor.astype(jnp.bfloat16)).astype(jnp.float32)

def reference(queries, keys, values, out_grad, segments):
    inv_root = 1.0 / math.sqrt(HDIM)
    pad_rows = REACH * TOK_DEV
    key_width = (REACH + 1) * TOK_DEV
    feature = HEADS * HDIM
    keys_padded = jnp.concatenate([jnp.zeros((pad_rows, feature), keys.dtype), keys], 0)
    values_padded = jnp.concatenate([jnp.zeros((pad_rows, feature), values.dtype), values], 0)
    seg_padded = jnp.concatenate([jnp.full((pad_rows,), -1, jnp.int32), segments.astype(jnp.int32)], 0)

    def one_block(carry, block_index):
        key_acc, value_acc = carry
        start = (block_index * TOK_DEV).astype(jnp.int32)
        query_block = lax.dynamic_slice_in_dim(queries, start, TOK_DEV, 0).reshape(TOK_DEV, HEADS, HDIM).astype(jnp.float32)
        grad_block = lax.dynamic_slice_in_dim(out_grad, start, TOK_DEV, 0).reshape(TOK_DEV, HEADS, HDIM).astype(jnp.float32)
        key_block = lax.dynamic_slice_in_dim(keys_padded, start, key_width, 0).reshape(key_width, HEADS, HDIM).astype(jnp.float32)
        value_block = lax.dynamic_slice_in_dim(values_padded, start, key_width, 0).reshape(key_width, HEADS, HDIM).astype(jnp.float32)
        query_seg = lax.dynamic_slice_in_dim(segments.astype(jnp.int32), start, TOK_DEV, 0)
        key_seg = lax.dynamic_slice_in_dim(seg_padded, start, key_width, 0)
        query_pos = start + jnp.arange(TOK_DEV, dtype=jnp.int32)
        key_pos = start - pad_rows + jnp.arange(key_width, dtype=jnp.int32)
        visible = (key_pos[None, :] <= query_pos[:, None]) & (key_seg[None, :] == query_seg[:, None])
        scores = jnp.einsum('ihd,jhd->hij', query_block, key_block) * inv_root
        scores = jnp.where(visible[None], scores, -jnp.inf)
        row_peak = lax.optimization_barrier(jnp.max(scores, -1, keepdims=True))
        exponent = jnp.exp(scores - row_peak)
        row_total = lax.optimization_barrier(jnp.sum(exponent, -1, keepdims=True))
        weights = to_half(exponent / row_total)
        attended = jnp.einsum('hij,jhd->ihd', weights, value_block).astype(jnp.bfloat16)
        dprob = jnp.einsum('ihd,jhd->hij', grad_block, value_block)
        row_delta = lax.optimization_barrier(jnp.sum(grad_block * attended.astype(jnp.float32), -1)).T
        dscore = to_half(weights * (dprob - row_delta[:, :, None]) * inv_root)
        query_grad = jnp.einsum('hij,jhd->ihd', dscore, key_block).astype(jnp.bfloat16)
        key_part = jnp.einsum('hij,ihd->jhd', dscore, query_block).reshape(key_width, feature)
        value_part = jnp.einsum('hij,ihd->jhd', weights, grad_block).reshape(key_width, feature)
        key_acc = lax.dynamic_update_slice_in_dim(key_acc, lax.dynamic_slice_in_dim(key_acc, start, key_width, 0) + key_part, start, 0)
        value_acc = lax.dynamic_update_slice_in_dim(value_acc, lax.dynamic_slice_in_dim(value_acc, start, key_width, 0) + value_part, start, 0)
        return ((key_acc, value_acc), (attended.reshape(TOK_DEV, feature), query_grad.reshape(TOK_DEV, feature)))
    zeros_acc = jnp.zeros((pad_rows + TOKENS, feature), jnp.float32)
    (key_acc, value_acc), (attended, query_grad) = lax.scan(one_block, (zeros_acc, zeros_acc), jnp.arange(TOKENS // TOK_DEV, dtype=jnp.int32))
    return (attended.reshape(TOKENS, feature), query_grad.reshape(TOKENS, feature), key_acc[pad_rows:].astype(jnp.bfloat16), value_acc[pad_rows:].astype(jnp.bfloat16))
```

```python
import functools
import math

import jax
import jax.numpy as jnp
from jax import lax
from jax.experimental import pallas as pl
from jax.experimental.pallas import tpu as pltpu
from jax.sharding import PartitionSpec as P

HEADS = 16
MESH = pl.DeviceIdType.MESH
DELAY = 3
NEG = -1e30
F32 = jnp.float32
BF16 = jnp.bfloat16


def dot_nt(a, b):
    return lax.dot_general(a, b, (((1,), (1,)), ((), ())), preferred_element_type=F32)


def dot_nn(a, b):
    return lax.dot_general(a, b, (((1,), (0,)), ((), ())), preferred_element_type=F32)


def dot_tn(a, b):
    return lax.dot_general(a, b, (((0,), (0,)), ((), ())), preferred_element_type=F32)


def colsum(x):
    return jnp.sum(x, axis=0, keepdims=True)


def colmax(x):
    return jnp.max(x, axis=0, keepdims=True)


def kernel(
    n,
    q_h, k_h, v_h, g_h, seg_h,
    o_h, dq_h, dk_h, dv_h,
    q_all, k_all, v_all, g_all, seg_buf, flags,
    b_own, b_left, b_right, b_far,
    rp, rm, sendp, sendm,
    st_own, st_in, st_tot, st_ret, st_fin,
    acc_o, acc_dq, acc_dk, acc_dv, staged,
    in_loc, in_snd, in_rcv, seg_sem,
    p_snd, p_rcv, m_snd, m_rcv,
    a_snd, a_rcv, f_snd, f_rcv,
    out_loc, out_snd, out_rcv,
):
    tok, feature = q_h.shape
    heads = HEADS // 2
    hd = feature // HEADS
    own = 2 * tok
    span = own - hd
    scale = math.log2(math.e) / math.sqrt(hd)
    inv_root = 1.0 / math.sqrt(hd)
    wide = 2 * hd

    me = lax.axis_index("seq")
    core = lax.rem(me, 2)
    partner = me + 1 - 2 * core
    left = lax.rem(me + n - 2, n)
    right = lax.rem(me + 2, n)

    barrier = pltpu.get_barrier_semaphore()
    for peer in (partner, left, right):
        pl.semaphore_signal(barrier, inc=1, device_id={"seq": peer}, device_id_type=MESH)
    pl.semaphore_wait(barrier, 3)

    def remote(src, dst, snd, rcv, peer):
        return pltpu.make_async_remote_copy(
            src_ref=src, dst_ref=dst, send_sem=snd, recv_sem=rcv,
            device_id={"seq": peer}, device_id_type=MESH,
        )

    mine = pl.ds(pl.multiple_of(core * tok, tok), tok)
    theirs = pl.ds(pl.multiple_of((1 - core) * tok, tok), tok)
    pairs_in = ((k_h, k_all), (v_h, v_all), (q_h, q_all), (g_h, g_all))

    def columns(which, h):
        return pl.ds(pl.multiple_of((which * heads + h) * hd, hd), hd)

    def in_local(j, h):
        src, dst = pairs_in[j]
        return pltpu.make_async_copy(src.at[:, columns(core, h)], dst.at[h, mine], in_loc.at[j, h])

    def in_remote(j, h):
        src, dst = pairs_in[j]
        return remote(
            src.at[:, columns(1 - core, h)], dst.at[h, mine], in_snd.at[j, h], in_rcv.at[j, h], partner
        )

    seg_local = pltpu.make_async_copy(seg_h, seg_buf.at[0, core], seg_sem.at[0])
    seg_remote = remote(seg_h, seg_buf.at[0, core], seg_sem.at[1], seg_sem.at[2], partner)
    seg_right = remote(seg_buf.at[0], seg_buf.at[1], seg_sem.at[3], seg_sem.at[4], right)
    seg_left = remote(seg_buf.at[0], seg_buf.at[2], seg_sem.at[5], seg_sem.at[6], left)
    seg_local.start()
    seg_remote.start()

    def start_inputs(h, _):
        for j in range(4):
            in_remote(j, h).start()
            in_local(j, h).start()
        return 0

    lax.fori_loop(0, heads, start_inputs, 0)

    def wait_inputs(h):
        for j in range(4):
            in_local(j, h).wait()
            in_remote(j, h).wait_recv()

    def early(t):
        tail, head = pl.ds(own - span, span), pl.ds(0, span)
        return (
            remote(k_all.at[t, tail], rp.at[t, 0], p_snd.at[t, 0], p_rcv.at[t, 0], right),
            remote(q_all.at[t, head], rm.at[t, 0], m_snd.at[t, 0], m_rcv.at[t, 0], left),
            remote(v_all.at[t, tail], rp.at[t, 1], p_snd.at[t, 1], p_rcv.at[t, 1], right),
            remote(g_all.at[t, head], rm.at[t, 1], m_snd.at[t, 1], m_rcv.at[t, 1], left),
        )

    def late(h):
        t = h + DELAY
        return (
            remote(sendp.at[h, 0], rp.at[t, 0], p_snd.at[t, 0], p_rcv.at[t, 0], right),
            remote(sendp.at[h, 1], rp.at[t, 1], p_snd.at[t, 1], p_rcv.at[t, 1], right),
            remote(st_ret.at[h], st_fin.at[h], f_snd.at[h], f_rcv.at[h], right),
            remote(sendm.at[h, 0], rm.at[t, 0], m_snd.at[t, 0], m_rcv.at[t, 0], left),
            remote(sendm.at[h, 1], rm.at[t, 1], m_snd.at[t, 1], m_rcv.at[t, 1], left),
        )

    def stats(h):
        return remote(st_own.at[h], st_in.at[h], a_snd.at[h], a_rcv.at[h], left)

    def start_early(t, _):
        wait_inputs(t)
        for copy in early(t):
            copy.start()
        return 0

    start_early(0, 0)
    seg_local.wait()
    seg_remote.wait_recv()
    seg_right.start()
    seg_left.start()
    lax.fori_loop(1, DELAY, start_early, 0)

    def rows(ref, h, first, blocks):
        parts = [ref[h, first + b : first + b + 1, :] for b in range(blocks)]
        return parts[0] if blocks == 1 else jnp.concatenate(parts, axis=1)

    def put_rows(ref, h, first, value):
        for b in range(value.shape[1] // hd):
            ref[h, first + b : first + b + 1, :] = value[:, b * hd : (b + 1) * hd]

    def own_stats(h):
        for b in range(2):
            depth = (b + 1) * wide
            at = slice(b * wide, (b + 1) * wide)
            s = dot_nt(k_all[h, :depth], q_all[h, at]) * scale + b_own[:depth, at]
            dp = dot_nt(v_all[h, :depth], g_all[h, at])
            m = colmax(s)
            p = jnp.exp2(s - m)
            total = colsum(p)
            put_rows(st_own, h, 2 * b, m + jnp.log2(total))
            put_rows(st_own, h, 4 + 2 * b, colsum(p * dp) / total)

    def finish(s, dp, lse, delta):
        p = jnp.exp2(s - lse)
        return p.astype(BF16), (p * ((dp - delta) * inv_root)).astype(BF16)

    def merge(lse, delta, parts):
        m = lse
        for s, _ in parts:
            m = jnp.maximum(m, colmax(s))
        first = jnp.exp2(lse - m)
        total, dn = first, delta * first
        probs = []
        for s, dp in parts:
            p = jnp.exp2(s - m)
            total = total + colsum(p)
            dn = dn + colsum(p * dp)
            probs.append(p)
        inv = 1.0 / total
        delta = dn * inv
        outs = []
        for p, (_, dp) in zip(probs, parts):
            p = p * inv
            outs.append((p.astype(BF16), (p * ((dp - delta) * inv_root)).astype(BF16)))
        return m + jnp.log2(total), delta, outs

    def cross(h):
        cut = span - wide
        nxt = jnp.minimum(h + DELAY, heads - 1)
        fresh = jnp.where(h + DELAY < heads, 1.0, 0.0)
        keys_right = jnp.broadcast_to((1.0 - flags[1:2, :]) * fresh, (span, hd)) > 0.5
        queries_left = jnp.broadcast_to(flags[0:1, :] * fresh, (span, hd)) > 0.5
        kl, vl = rp[h, 0], rp[h, 1]
        k, v = k_all[h], v_all[h]
        qa, ga = rm[h, 0, :wide], rm[h, 1, :wide]
        s1 = dot_nt(k, qa) * scale + b_right[:, :wide]
        s2 = dot_nt(kl[cut:], qa) * scale + b_far[...]
        d1, d2 = dot_nt(v, ga), dot_nt(vl[cut:], ga)
        lse, delta, ((p1, e1), (p2, e2)) = merge(
            rows(st_in, h, 0, 2), rows(st_in, h, 4, 2), ((s1, d1), (s2, d2))
        )
        put_rows(st_ret, h, 0, lse)
        put_rows(st_ret, h, 4, delta)
        dk, dv = dot_nn(e1, qa), dot_nn(p1, ga)
        dkl, dvl = dot_nn(e2, qa), dot_nn(p2, ga)
        for i, (a1, b1, a2, b2, kept) in enumerate(
            ((p1, v, p2, vl[cut:], k_all), (e1, k, e2, kl[cut:], v_all))
        ):
            part = dot_tn(a1, b1) + dot_tn(a2, b2)
            stay = kept[nxt, own - span : own - span + wide].astype(F32)
            sendp[h, i, :wide] = jnp.where(keys_right[:wide], stay, part).astype(BF16)
        qb, gb = rm[h, 0, wide:], rm[h, 1, wide:]
        s3 = dot_nt(k, qb) * scale + b_right[:, wide:]
        d3 = dot_nt(v, gb)
        lse, delta, ((p3, e3),) = merge(rows(st_in, h, 2, 1), rows(st_in, h, 6, 1), ((s3, d3),))
        put_rows(st_ret, h, 2, lse)
        put_rows(st_ret, h, 6, delta)
        acc_dk[h] = dk + dot_nn(e3, qb)
        acc_dv[h] = dv + dot_nn(p3, gb)
        for i, (a3, b3, kept) in enumerate(((p3, v, k_all), (e3, k, v_all))):
            part = dot_tn(a3, b3)
            stay = kept[nxt, own - span + wide :].astype(F32)
            sendp[h, i, wide:] = jnp.where(keys_right[wide:], stay, part).astype(BF16)
        dkl_sum = dvl_sum = None
        for b in range(2):
            at = slice(b * wide, (b + 1) * wide)
            q, g = q_all[h, at], g_all[h, at]
            s = dot_nt(kl, q) * scale + b_left[:, at]
            dp = dot_nt(vl, g)
            lse, delta, ((p, e),) = merge(
                rows(st_own, h, 2 * b, 2), rows(st_own, h, 4 + 2 * b, 2), ((s, dp),)
            )
            put_rows(st_tot, h, 2 * b, lse)
            put_rows(st_tot, h, 4 + 2 * b, delta)
            acc_o[h, at] = dot_tn(p, vl)
            acc_dq[h, at] = dot_tn(e, kl)
            dkb, dvb = dot_nn(e, q), dot_nn(p, g)
            dkl_sum = dkb if b == 0 else dkl_sum + dkb
            dvl_sum = dvb if b == 0 else dvl_sum + dvb
        for i, (total, extra, kept) in enumerate(((dkl_sum, dkl, q_all), (dvl_sum, dvl, g_all))):
            stay = kept[nxt, :span].astype(F32)
            sendm[h, i, :cut] = jnp.where(queries_left[:cut], stay[:cut], total[:cut]).astype(BF16)
            sendm[h, i, cut:] = jnp.where(
                queries_left[cut:], stay[cut:], total[cut:] + extra
            ).astype(BF16)

    def close(h):
        t = h + DELAY
        asked = flags[0:1, :] > 0.5
        back = jnp.broadcast_to(flags[0:1, :], (span, hd)) > 0.5
        back_keys = jnp.broadcast_to(1.0 - flags[1:2, :], (span, hd)) > 0.5
        lse = [st_tot[h, b : b + 1, :] for b in range(4)]
        delta = [st_tot[h, 4 + b : 5 + b, :] for b in range(4)]
        for b in range(3):
            lse[b] = jnp.where(asked, st_fin[h, b : b + 1, :], lse[b])
            delta[b] = jnp.where(asked, st_fin[h, 4 + b : 5 + b, :], delta[b])
        add = [jnp.where(back, rp[t, i].astype(F32), 0.0) for i in range(2)]
        for b in range(2):
            depth = (b + 1) * wide
            at = slice(b * wide, (b + 1) * wide)
            q, g, k, v = q_all[h, at], g_all[h, at], k_all[h, :depth], v_all[h, :depth]
            s = dot_nt(k, q) * scale + b_own[:depth, at]
            dp = dot_nt(v, g)
            p, e = finish(
                s, dp, jnp.concatenate(lse[2 * b : 2 * b + 2], 1), jnp.concatenate(delta[2 * b : 2 * b + 2], 1)
            )
            acc_dk[h, :depth] += dot_nn(e, q)
            acc_dv[h, :depth] += dot_nn(p, g)
            for i, (value, acc) in enumerate(((dot_tn(p, v), acc_o), (dot_tn(e, k), acc_dq))):
                value = value + acc[h, at]
                if b == 0:
                    staged[h, i, at] = (value + add[i][:wide]).astype(BF16)
                else:
                    staged[h, i, wide:span] = (value[: span - wide] + add[i][wide:]).astype(BF16)
                    staged[h, i, span:] = value[span - wide :].astype(BF16)
        for i, acc in ((0, acc_dk), (1, acc_dv)):
            staged[h, 2 + i, : own - span] = acc[h, : own - span].astype(BF16)
            staged[h, 2 + i, own - span :] = (
                acc[h, own - span :] + jnp.where(back_keys, rm[t, i].astype(F32), 0.0)
            ).astype(BF16)

    outs = (o_h, dq_h, dk_h, dv_h)

    def out_local(j, h):
        return pltpu.make_async_copy(
            staged.at[h, j, mine], outs[j].at[:, columns(core, h)], out_loc.at[j, h]
        )

    def out_remote(j, h):
        return remote(
            staged.at[h, j, theirs], outs[j].at[:, columns(core, h)],
            out_snd.at[j, h], out_rcv.at[j, h], partner,
        )

    seg_right.wait_recv()
    seg_left.wait_recv()

    def seg_row(chip, b):
        return seg_buf[chip, b // 2, b % 2 : b % 2 + 1, :].astype(F32)

    def seg_at(chip, b, lane):
        return jnp.broadcast_to(seg_row(chip, b)[:, lane : lane + 1], (1, hd))

    asks_left = seg_at(1, 0, hd - 1) == seg_at(0, 0, 0)
    asks_right = seg_at(0, 0, hd - 1) == seg_at(2, 0, 0)
    flags[0:1, :] = jnp.where(asks_left, 1.0, 0.0)
    flags[1:2, :] = jnp.where(asks_right, 1.0, 0.0)

    def as_column(row):
        return jnp.transpose(jnp.broadcast_to(row, (hd, hd)))

    own_rows = [seg_row(0, b) for b in range(4)]
    own_cols = [as_column(row) for row in own_rows]
    left_cols = [as_column(jnp.where(asks_left, -1.0, seg_row(1, b + 1))) for b in range(3)]
    right_rows = [jnp.where(asks_right, seg_row(2, b), -2.0) for b in range(3)]
    causal = lax.broadcasted_iota(jnp.int32, (hd, hd), 0) <= lax.broadcasted_iota(jnp.int32, (hd, hd), 1)

    def tile(a, b):
        return slice(a * hd, (a + 1) * hd), slice(b * hd, (b + 1) * hd)

    for a in range(4):
        for b in range(4):
            if a > b:
                b_own[tile(a, b)] = jnp.full((hd, hd), NEG, F32)
            else:
                same = own_cols[a] == own_rows[b]
                b_own[tile(a, b)] = jnp.where(same & causal if a == b else same, 0.0, NEG)
            if a < 3:
                b_left[tile(a, b)] = jnp.where(left_cols[a] == own_rows[b], 0.0, NEG)
            if b < 3:
                b_right[tile(a, b)] = jnp.where(own_cols[a] == right_rows[b], 0.0, NEG)
            if a < 2 and b < 2:
                b_far[tile(a, b)] = jnp.where(left_cols[a + 1] == right_rows[b], 0.0, NEG)

    own_stats(0)
    stats(0).start()

    def step(i, _):
        @pl.when(i + 1 < heads)
        def _():
            own_stats(i + 1)
            stats(i + 1).start()

        @pl.when(i + DELAY < heads)
        def _():
            wait_inputs(i + DELAY)

        for j in range(2):
            remote(sendp.at[0, j], rp.at[i, j], p_snd.at[i, j], p_rcv.at[i, j], right).wait_recv()
            remote(sendm.at[0, j], rm.at[i, j], m_snd.at[i, j], m_rcv.at[i, j], left).wait_recv()

        @pl.when(i < heads)
        def _():
            stats(i).wait_recv()
            cross(i)
            for copy in late(i):
                copy.start()

        @pl.when(i >= DELAY)
        def _():
            h = i - DELAY
            remote(st_ret.at[h], st_fin.at[h], f_snd.at[h], f_rcv.at[h], right).wait_recv()
            close(h)
            for j in range(4):
                out_remote(j, h).start()
                out_local(j, h).start()

        return 0

    lax.fori_loop(0, heads + DELAY, step, 0)

    def drain(h, _):
        for j in range(4):
            in_remote(j, h).wait_send()
            out_local(j, h).wait()
            out_remote(j, h).wait()
        stats(h).wait_send()
        for copy in late(h):
            copy.wait_send()
        return 0

    def drain_early(t, _):
        for copy in early(t):
            copy.wait_send()
        return 0

    lax.fori_loop(0, heads, drain, 0)
    lax.fori_loop(0, DELAY, drain_early, 0)
    seg_remote.wait_send()
    seg_right.wait_send()
    seg_left.wait_send()


def local(n, queries, keys, values, out_grad, segments):
    tok, feature = queries.shape
    heads, hd = HEADS // 2, feature // HEADS
    own = 2 * tok
    span = own - hd
    slots = heads + DELAY
    out = jax.ShapeDtypeStruct((tok, feature), BF16)
    dma = pltpu.SemaphoreType.DMA
    vm = pltpu.VMEM
    return pl.pallas_call(
        functools.partial(kernel, n),
        out_shape=(out,) * 4,
        in_specs=[pl.BlockSpec(memory_space=pl.ANY)] * 5,
        out_specs=[pl.BlockSpec(memory_space=pl.ANY)] * 4,
        scratch_shapes=[
            vm((heads, own, hd), BF16), vm((heads, own, hd), BF16),
            vm((heads, own, hd), BF16), vm((heads, own, hd), BF16),
            vm((3, 2, 2, hd), jnp.int32), vm((8, hd), F32),
            vm((own, own), F32), vm((span, own), F32), vm((own, span), F32), vm((2 * hd, 2 * hd), F32),
            vm((slots, 2, span, hd), BF16), vm((slots, 2, span, hd), BF16),
            vm((heads, 2, span, hd), BF16), vm((heads, 2, span, hd), BF16),
            vm((heads, 8, hd), F32), vm((heads, 8, hd), F32), vm((heads, 8, hd), F32),
            vm((heads, 8, hd), F32), vm((heads, 8, hd), F32),
            vm((heads, own, hd), F32), vm((heads, own, hd), F32),
            vm((heads, own, hd), F32), vm((heads, own, hd), F32),
            vm((heads, 4, own, hd), BF16),
            dma((4, heads)), dma((4, heads)), dma((4, heads)), dma((7,)),
            dma((slots, 2)), dma((slots, 2)), dma((slots, 2)), dma((slots, 2)),
            dma((heads,)), dma((heads,)), dma((heads,)), dma((heads,)),
            dma((4, heads)), dma((4, heads)), dma((4, heads)),
        ],
        compiler_params=pltpu.CompilerParams(
            collective_id=0, has_side_effects=True, vmem_limit_bytes=60 * 2**20
        ),
        name="packed_attention",
    )(queries, keys, values, out_grad, segments.reshape(2, tok // 2))


def solution(mesh):
    spec = P(("branch", "seq"), None)
    return jax.shard_map(
        functools.partial(local, mesh.shape["seq"]),
        mesh=mesh,
        in_specs=(spec,) * 4 + (P(("branch", "seq")),),
        out_specs=(spec,) * 4,
        check_vma=False,
    )
```

```python
import functools
import math

import jax
import jax.numpy as jnp
from jax import lax
from jax.experimental import pallas as pl
from jax.experimental.pallas import tpu as pltpu
from jax.sharding import PartitionSpec as P

HEADS = 16
MESH = pl.DeviceIdType.MESH
DELAY = 2
NEG = -1e30
STAT = 16
F32 = jnp.float32
BF16 = jnp.bfloat16


def dot_nt(a, b):
    return lax.dot_general(a, b, (((1,), (1,)), ((), ())), preferred_element_type=F32)


def dot_nn(a, b):
    return lax.dot_general(a, b, (((1,), (0,)), ((), ())), preferred_element_type=F32)


def dot_tn(a, b):
    return lax.dot_general(a, b, (((0,), (0,)), ((), ())), preferred_element_type=F32)


def colsum(x):
    return jnp.sum(x, axis=0, keepdims=True)


def colmax(x):
    return jnp.max(x, axis=0, keepdims=True)


def kernel(
    n,
    q_h, k_h, v_h, g_h, seg_h,
    o_h, dq_h, dk_h, dv_h,
    q_all, k_all, v_all, g_all, seg_buf, flags,
    b_own, b_left, b_right, b_far,
    rp, rm, sendp, sendm, first,
    st_own, st_tot,
    acc_o, acc_dq, acc_dk, acc_dv, staged,
    in_loc, in_snd, in_rcv, seg_sem,
    e_snd, e_rcv, l_snd, l_rcv,
    out_snd, out_rcv,
):
    tok, feature = q_h.shape
    heads = HEADS // 2
    hd = feature // HEADS
    own = 2 * tok
    span = own - hd
    scale = math.log2(math.e) / math.sqrt(hd)
    inv_root = 1.0 / math.sqrt(hd)
    wide = 2 * hd

    def col(h, count=1):
        start = h * hd if isinstance(h, int) else pl.multiple_of(h * hd, hd)
        return pl.ds(start, count * hd)

    me = lax.axis_index("seq")
    core = lax.rem(me, 2)
    partner = me + 1 - 2 * core
    left = lax.rem(me + n - 2, n)
    right = lax.rem(me + 2, n)

    barrier = pltpu.get_barrier_semaphore()
    for peer in (partner, left, right):
        pl.semaphore_signal(barrier, inc=1, device_id={"seq": peer}, device_id_type=MESH)
    pl.semaphore_wait(barrier, 3)

    def remote(src, dst, snd, rcv, peer):
        return pltpu.make_async_remote_copy(
            src_ref=src, dst_ref=dst, send_sem=snd, recv_sem=rcv,
            device_id={"seq": peer}, device_id_type=MESH,
        )

    mine = pl.ds(pl.multiple_of(core * tok, tok), tok)
    theirs = pl.ds(pl.multiple_of((1 - core) * tok, tok), tok)
    pairs_in = ((k_h, k_all), (v_h, v_all), (q_h, q_all), (g_h, g_all))

    def group(which, s):
        return col(which * heads + s, 1 if s < DELAY else heads - DELAY)

    def in_local(j, s):
        src, dst = pairs_in[j]
        return pltpu.make_async_copy(src.at[:, group(core, s)], dst.at[mine, group(0, s)], in_loc.at[j, s])

    def in_remote(j, s):
        src, dst = pairs_in[j]
        return remote(
            src.at[:, group(1 - core, s)], dst.at[mine, group(0, s)], in_snd.at[j, s], in_rcv.at[j, s], partner
        )

    seg_local = pltpu.make_async_copy(seg_h, seg_buf.at[0, core], seg_sem.at[0])
    seg_remote = remote(seg_h, seg_buf.at[0, core], seg_sem.at[1], seg_sem.at[2], partner)
    seg_right = remote(seg_buf.at[0], seg_buf.at[1], seg_sem.at[3], seg_sem.at[4], right)
    seg_left = remote(seg_buf.at[0], seg_buf.at[2], seg_sem.at[5], seg_sem.at[6], left)
    for s in range(DELAY + 1):
        for j in range(4):
            in_remote(j, s).start()
            in_local(j, s).start()
        if s == 0:
            seg_local.start()
            seg_remote.start()

    tail, head, below = pl.ds(own - span, span), pl.ds(0, span), pl.ds(2 * span, STAT)

    def early(t, i):
        src, dst, peer = (
            (k_all.at[tail, col(t)], rp.at[t, pl.ds(0, span)], right),
            (q_all.at[head, col(t)], rm.at[t, pl.ds(0, span)], left),
            (v_all.at[tail, col(t)], rp.at[t, pl.ds(span, span)], right),
            (g_all.at[head, col(t)], rm.at[t, pl.ds(span, span)], left),
            (first.at[t], rm.at[t, below], left),
        )[i]
        return remote(src, dst, e_snd.at[t, i], e_rcv.at[t, i], peer)

    def to_right(h):
        return remote(sendp.at[h], rp.at[h + DELAY], l_snd.at[0, h], l_rcv.at[0, h], right)

    def to_left(h):
        return remote(sendm.at[h], rm.at[h + DELAY], l_snd.at[1, h], l_rcv.at[1, h], left)

    def start_early(t):
        for i, j in enumerate((0, 2, 1, 3)):
            in_local(j, t).wait()
            in_remote(j, t).wait_recv()
            early(t, i).start()

    start_early(0)
    seg_local.wait()
    seg_remote.wait_recv()
    seg_right.start()
    seg_left.start()

    def rows(ref, h, at, blocks):
        parts = [ref[h, at + b : at + b + 1, :] for b in range(blocks)]
        return parts[0] if blocks == 1 else jnp.concatenate(parts, axis=1)

    def put_rows(ref, h, at, value):
        for b in range(value.shape[1] // hd):
            ref[h, at + b : at + b + 1, :] = value[:, b * hd : (b + 1) * hd]

    def encode(lse, delta):
        out = []
        for row in lse:
            top = row.astype(BF16).astype(F32)
            mid = (row - top).astype(BF16).astype(F32)
            out += [top, mid, row - top - mid]
        for row in delta:
            top = row.astype(BF16).astype(F32)
            out += [top, row - top]
        out.append(jnp.zeros_like(out[0]))
        return jnp.concatenate(out, axis=0).astype(BF16)

    def decode(ref, t):
        table = ref[t, 2 * span : 2 * span + STAT, :].astype(F32)
        lse = [table[3 * b : 3 * b + 1] + table[3 * b + 1 : 3 * b + 2] + table[3 * b + 2 : 3 * b + 3] for b in range(3)]
        delta = [table[9 + 2 * b : 10 + 2 * b] + table[10 + 2 * b : 11 + 2 * b] for b in range(3)]
        return lse, delta

    def own_stats(h):
        lses, deltas = [], []
        for b in range(2):
            depth = (b + 1) * wide
            at = slice(b * wide, (b + 1) * wide)
            s = dot_nt(k_all[:depth, col(h)], q_all[at, col(h)]) * scale + b_own[:depth, at]
            dp = dot_nt(v_all[:depth, col(h)], g_all[at, col(h)])
            m = colmax(s)
            p = jnp.exp2(s - m)
            total = colsum(p)
            lse, delta = m + jnp.log2(total), colsum(p * dp) / total
            put_rows(st_own, h, 2 * b, lse)
            put_rows(st_own, h, 4 + 2 * b, delta)
            lses += [lse[:, :hd], lse[:, hd:]]
            deltas += [delta[:, :hd], delta[:, hd:]]
        return encode(lses[:3], deltas[:3])

    def finish(s, dp, lse, delta):
        p = jnp.exp2(s - lse)
        return p.astype(BF16), (p * ((dp - delta) * inv_root)).astype(BF16)

    def merge(lse, delta, parts):
        m = lse
        for s, _ in parts:
            m = jnp.maximum(m, colmax(s))
        first = jnp.exp2(lse - m)
        total, dn = first, delta * first
        probs = []
        for s, dp in parts:
            p = jnp.exp2(s - m)
            total = total + colsum(p)
            dn = dn + colsum(p * dp)
            probs.append(p)
        inv = 1.0 / total
        delta = dn * inv
        outs = []
        for p, (_, dp) in zip(probs, parts):
            p = p * inv
            outs.append((p.astype(BF16), (p * ((dp - delta) * inv_root)).astype(BF16)))
        return m + jnp.log2(total), delta, outs

    def cross(h):
        cut = span - wide
        nxt = jnp.minimum(h + DELAY, heads - 1)
        fresh = jnp.where(h + DELAY < heads, 1.0, 0.0)
        keys_right = jnp.broadcast_to((1.0 - flags[1:2, :]) * fresh, (span, hd)) > 0.5
        queries_left = jnp.broadcast_to(flags[0:1, :] * fresh, (span, hd)) > 0.5
        kl, vl = rp[h, :span], rp[h, span : 2 * span]
        lse_in, delta_in = decode(rm, h)
        k, v = k_all[:, col(h)], v_all[:, col(h)]
        qa, ga = rm[h, :wide], rm[h, span : span + wide]
        s1 = dot_nt(k, qa) * scale + b_right[:, :wide]
        s2 = dot_nt(kl[cut:], qa) * scale + b_far[...]
        d1, d2 = dot_nt(v, ga), dot_nt(vl[cut:], ga)
        lse, delta, ((p1, e1), (p2, e2)) = merge(
            jnp.concatenate(lse_in[:2], 1), jnp.concatenate(delta_in[:2], 1), ((s1, d1), (s2, d2))
        )
        lse_out, delta_out = [lse[:, :hd], lse[:, hd:]], [delta[:, :hd], delta[:, hd:]]
        dk, dv = dot_nn(e1, qa), dot_nn(p1, ga)
        dkl, dvl = dot_nn(e2, qa), dot_nn(p2, ga)
        for i, (a1, b1, a2, b2, kept) in enumerate(
            ((p1, v, p2, vl[cut:], k_all), (e1, k, e2, kl[cut:], v_all))
        ):
            part = dot_tn(a1, b1) + dot_tn(a2, b2)
            stay = kept[own - span : own - span + wide, col(nxt)].astype(F32)
            sendp[h, i * span : i * span + wide] = jnp.where(keys_right[:wide], stay, part).astype(BF16)
        qb, gb = rm[h, wide:span], rm[h, span + wide : 2 * span]
        s3 = dot_nt(k, qb) * scale + b_right[:, wide:]
        d3 = dot_nt(v, gb)
        lse, delta, ((p3, e3),) = merge(lse_in[2], delta_in[2], ((s3, d3),))
        sendp[h, 2 * span :] = encode(lse_out + [lse], delta_out + [delta])
        acc_dk[h] = dk + dot_nn(e3, qb)
        acc_dv[h] = dv + dot_nn(p3, gb)
        for i, (a3, b3, kept) in enumerate(((p3, v, k_all), (e3, k, v_all))):
            part = dot_tn(a3, b3)
            stay = kept[own - span + wide :, col(nxt)].astype(F32)
            sendp[h, i * span + wide : (i + 1) * span] = jnp.where(keys_right[wide:], stay, part).astype(BF16)
        to_right(h).start()
        dkl_sum = dvl_sum = None
        for b in range(2):
            at = slice(b * wide, (b + 1) * wide)
            q, g = q_all[at, col(h)], g_all[at, col(h)]
            s = dot_nt(kl, q) * scale + b_left[:, at]
            dp = dot_nt(vl, g)
            lse, delta, ((p, e),) = merge(
                rows(st_own, h, 2 * b, 2), rows(st_own, h, 4 + 2 * b, 2), ((s, dp),)
            )
            put_rows(st_tot, h, 2 * b, lse)
            put_rows(st_tot, h, 4 + 2 * b, delta)
            acc_o[h, at] = dot_tn(p, vl)
            acc_dq[h, at] = dot_tn(e, kl)
            dkb, dvb = dot_nn(e, q), dot_nn(p, g)
            dkl_sum = dkb if b == 0 else dkl_sum + dkb
            dvl_sum = dvb if b == 0 else dvl_sum + dvb
        for i, (total, extra, kept) in enumerate(((dkl_sum, dkl, q_all), (dvl_sum, dvl, g_all))):
            stay = kept[:span, col(nxt)].astype(F32)
            sendm[h, i * span : i * span + cut] = jnp.where(queries_left[:cut], stay[:cut], total[:cut]).astype(BF16)
            sendm[h, i * span + cut : (i + 1) * span] = jnp.where(
                queries_left[cut:], stay[cut:], total[cut:] + extra
            ).astype(BF16)

    def close(h):
        t = h + DELAY
        asked = flags[0:1, :] > 0.5
        back = jnp.broadcast_to(flags[0:1, :], (span, hd)) > 0.5
        back_keys = jnp.broadcast_to(1.0 - flags[1:2, :], (span, hd)) > 0.5
        lse = [st_tot[h, b : b + 1, :] for b in range(4)]
        delta = [st_tot[h, 4 + b : 5 + b, :] for b in range(4)]
        lse_back, delta_back = decode(rp, t)
        for b in range(3):
            lse[b] = jnp.where(asked, lse_back[b], lse[b])
            delta[b] = jnp.where(asked, delta_back[b], delta[b])
        add = [jnp.where(back, rp[t, i * span : (i + 1) * span].astype(F32), 0.0) for i in range(2)]
        for b in range(2):
            depth = (b + 1) * wide
            at = slice(b * wide, (b + 1) * wide)
            q, g = q_all[at, col(h)], g_all[at, col(h)]
            k, v = k_all[:depth, col(h)], v_all[:depth, col(h)]
            s = dot_nt(k, q) * scale + b_own[:depth, at]
            dp = dot_nt(v, g)
            p, e = finish(
                s, dp, jnp.concatenate(lse[2 * b : 2 * b + 2], 1), jnp.concatenate(delta[2 * b : 2 * b + 2], 1)
            )
            acc_dk[h, :depth] += dot_nn(e, q)
            acc_dv[h, :depth] += dot_nn(p, g)
            for i, (value, acc) in enumerate(((dot_tn(p, v), acc_o), (dot_tn(e, k), acc_dq))):
                value = value + acc[h, at]
                if b == 0:
                    staged[h, i, at] = (value + add[i][:wide]).astype(BF16)
                else:
                    staged[h, i, wide:span] = (value[: span - wide] + add[i][wide:]).astype(BF16)
                    staged[h, i, span:] = value[span - wide :].astype(BF16)
        for i, acc in ((0, acc_dk), (1, acc_dv)):
            staged[h, 2 + i, : own - span] = acc[h, : own - span].astype(BF16)
            staged[h, 2 + i, own - span :] = (
                acc[h, own - span :] + jnp.where(back_keys, rm[t, i * span : (i + 1) * span].astype(F32), 0.0)
            ).astype(BF16)

    outs = (o_h, dq_h, dk_h, dv_h)

    def out_remote(j, h):
        return remote(
            staged.at[h, j, theirs], outs[j].at[:, col(core * heads + h)],
            out_snd.at[j, h], out_rcv.at[j, h], partner,
        )

    def seg_row(chip, b):
        return seg_buf[chip, b // 2, b % 2 : b % 2 + 1, :].astype(F32)

    def as_column(row):
        return jnp.transpose(jnp.broadcast_to(row, (hd, hd)))

    def tile(a, b):
        return slice(a * hd, (a + 1) * hd), slice(b * hd, (b + 1) * hd)

    own_rows = [seg_row(0, b) for b in range(4)]
    own_cols = [as_column(row) for row in own_rows]
    causal = lax.broadcasted_iota(jnp.int32, (hd, hd), 0) <= lax.broadcasted_iota(jnp.int32, (hd, hd), 1)
    for a in range(4):
        for b in range(4):
            same = own_cols[a] == own_rows[b]
            if a > b:
                b_own[tile(a, b)] = jnp.full((hd, hd), NEG, F32)
            else:
                b_own[tile(a, b)] = jnp.where(same & causal if a == b else same, 0.0, NEG)

    first[0] = own_stats(0)
    early(0, 4).start()
    for t in range(1, DELAY):
        start_early(t)
        first[t] = own_stats(t)
        early(t, 4).start()

    seg_right.wait_recv()
    seg_left.wait_recv()

    def seg_at(chip, b, lane):
        return jnp.broadcast_to(seg_row(chip, b)[:, lane : lane + 1], (1, hd))

    asks_left = seg_at(1, 0, hd - 1) == seg_at(0, 0, 0)
    asks_right = seg_at(0, 0, hd - 1) == seg_at(2, 0, 0)
    flags[0:1, :] = jnp.where(asks_left, 1.0, 0.0)
    flags[1:2, :] = jnp.where(asks_right, 1.0, 0.0)
    left_cols = [as_column(jnp.where(asks_left, -1.0, seg_row(1, b + 1))) for b in range(3)]
    right_rows = [jnp.where(asks_right, seg_row(2, b), -2.0) for b in range(3)]
    for a in range(4):
        for b in range(4):
            if a < 3:
                b_left[tile(a, b)] = jnp.where(left_cols[a] == own_rows[b], 0.0, NEG)
            if b < 3:
                b_right[tile(a, b)] = jnp.where(own_cols[a] == right_rows[b], 0.0, NEG)
            if a < 2 and b < 2:
                b_far[tile(a, b)] = jnp.where(left_cols[a + 1] == right_rows[b], 0.0, NEG)

    def step(i, _):
        @pl.when(i == 0)
        def _():
            for j in range(4):
                in_local(j, DELAY).wait()
                in_remote(j, DELAY).wait_recv()

        @pl.when(i + DELAY < heads)
        def _():
            sendm[i, 2 * span :] = own_stats(i + DELAY)

        @pl.when(i >= heads - DELAY)
        def _():
            @pl.when(i < heads)
            def _():
                sendm[i, 2 * span :] = jnp.zeros((STAT, hd), BF16)

        @pl.when(i < DELAY)
        def _():
            for j in range(5):
                early(i, j).wait()

        @pl.when(i >= DELAY)
        def _():
            to_right(i - DELAY).wait()
            to_left(i - DELAY).wait()

        @pl.when(i < heads)
        def _():
            cross(i)
            to_left(i).start()

        @pl.when(i >= DELAY)
        def _():
            h = i - DELAY
            close(h)
            for j in range(4):
                out_remote(j, h).start()
            for j in range(4):
                outs[j][:, col(core * heads + h)] = staged[h, j, mine, :]

        @pl.when(i > DELAY)
        def _():
            for j in range(4):
                out_remote(j, i - DELAY - 1).wait()

        return 0

    lax.fori_loop(0, heads + DELAY, step, 0)
    for s in range(DELAY + 1):
        for j in range(4):
            in_remote(j, s).wait_send()
    for j in range(4):
        out_remote(j, heads - 1).wait()
    seg_remote.wait_send()
    seg_right.wait_send()
    seg_left.wait_send()


def store(*refs):
    sem = refs[8]
    copies = [pltpu.make_async_copy(refs[j], refs[4 + j], sem.at[j]) for j in range(4)]
    for copy in copies:
        copy.start()
    for copy in copies:
        copy.wait()


def local(n, queries, keys, values, out_grad, segments):
    tok, feature = queries.shape
    heads, hd = HEADS // 2, feature // HEADS
    own = 2 * tok
    span = own - hd
    slots = heads + DELAY
    rows = 2 * span + STAT
    out = jax.ShapeDtypeStruct((tok, feature), BF16)
    dma = pltpu.SemaphoreType.DMA
    vm = pltpu.VMEM
    results = pl.pallas_call(
        functools.partial(kernel, n),
        out_shape=(vm((tok, feature), BF16),) * 4,
        in_specs=[pl.BlockSpec(memory_space=pltpu.HBM)] * 5,
        out_specs=[pl.BlockSpec(memory_space=vm)] * 4,
        scratch_shapes=[
            vm((own, heads * hd), BF16), vm((own, heads * hd), BF16),
            vm((own, heads * hd), BF16), vm((own, heads * hd), BF16),
            vm((3, 2, 2, hd), jnp.int32), vm((8, hd), F32),
            vm((own, own), F32), vm((span, own), F32), vm((own, span), F32), vm((2 * hd, 2 * hd), F32),
            vm((slots, rows, hd), BF16), vm((slots, rows, hd), BF16),
            vm((heads, rows, hd), BF16), vm((heads, rows, hd), BF16), vm((DELAY, STAT, hd), BF16),
            vm((heads, 8, hd), F32), vm((heads, 8, hd), F32),
            vm((heads, own, hd), F32), vm((heads, own, hd), F32),
            vm((heads, own, hd), F32), vm((heads, own, hd), F32),
            vm((heads, 4, own, hd), BF16),
            dma((4, DELAY + 1)), dma((4, DELAY + 1)), dma((4, DELAY + 1)), dma((7,)),
            dma((DELAY, 5)), dma((DELAY, 5)), dma((2, heads)), dma((2, heads)),
            dma((4, heads)), dma((4, heads)),
        ],
        compiler_params=pltpu.CompilerParams(
            collective_id=0, has_side_effects=True, vmem_limit_bytes=51 * 2**20
        ),
        name="packed_attention",
    )(*(pltpu.with_memory_space_constraint(x, pltpu.HBM) for x in (queries, keys, values, out_grad)), segments.reshape(2, tok // 2))
    return pl.pallas_call(
        store,
        out_shape=(out,) * 4,
        in_specs=[pl.BlockSpec(memory_space=pl.ANY)] * 4,
        out_specs=[pl.BlockSpec(memory_space=pl.ANY)] * 4,
        scratch_shapes=[dma((4,))],
        compiler_params=pltpu.CompilerParams(vmem_limit_bytes=2**20),
        name="store_results",
    )(*(pltpu.with_memory_space_constraint(r, vm) for r in results))


def solution(mesh):
    spec = P(("branch", "seq"), None)
    return jax.shard_map(
        functools.partial(local, mesh.shape["seq"]),
        mesh=mesh,
        in_specs=(spec,) * 4 + (P(("branch", "seq")),),
        out_specs=(spec,) * 4,
        check_vma=False,
    )
```

```python
import functools
import math

import jax
import jax.numpy as jnp
from jax import lax
from jax.experimental import pallas as pl
from jax.experimental.pallas import tpu as pltpu
from jax.sharding import PartitionSpec as P

HEADS = 16
MESH = pl.DeviceIdType.MESH
DELAY = 2
NEG = -1e30
STAT = 16
F32 = jnp.float32
BF16 = jnp.bfloat16


def dot_nt(a, b):
    return lax.dot_general(a, b, (((1,), (1,)), ((), ())), preferred_element_type=F32)


def dot_nn(a, b):
    return lax.dot_general(a, b, (((1,), (0,)), ((), ())), preferred_element_type=F32)


def dot_tn(a, b):
    return lax.dot_general(a, b, (((0,), (0,)), ((), ())), preferred_element_type=F32)


def colsum(x):
    return jnp.sum(x, axis=0, keepdims=True)


def colmax(x):
    return jnp.max(x, axis=0, keepdims=True)


def kernel(
    n,
    q_h, k_h, v_h, g_h, seg_h,
    o_h, dq_h, dk_h, dv_h,
    q_all, k_all, v_all, g_all, seg_buf, flags,
    b_own, b_left, b_right, b_far,
    rp, rm, sendp, sendm, first,
    st_own, st_tot,
    acc_o, acc_dq, acc_dk, acc_dv, staged,
    in_loc, in_snd, in_rcv, seg_sem,
    r_snd, r_rcv, e_snd, e_rcv, l_snd, l_rcv, ready,
    out_snd, out_rcv,
):
    tok, feature = q_h.shape
    heads = HEADS // 2
    hd = feature // HEADS
    own = 2 * tok
    span = own - hd
    scale = math.log2(math.e) / math.sqrt(hd)
    inv_root = 1.0 / math.sqrt(hd)
    wide = 2 * hd

    def col(h, count=1):
        start = h * hd if isinstance(h, int) else pl.multiple_of(h * hd, hd)
        return pl.ds(start, count * hd)

    me = lax.axis_index("seq")
    core = lax.rem(me, 2)
    partner = me + 1 - 2 * core
    chip = lax.div(me, 2)
    left = lax.rem(me + n - 2, n)
    right = lax.rem(me + 2, n)
    has_left = chip > 0
    has_right = chip < n // 2 - 1

    barrier = pltpu.get_barrier_semaphore()

    def signal(sem, peer):
        pl.semaphore_signal(sem, inc=1, device_id={"seq": peer}, device_id_type=MESH)

    @pl.when(has_left)
    def _():
        for c in range(2):
            signal(barrier, 2 * lax.div(left, 2) + c)

    @pl.when((core == 1) | jnp.logical_not(has_right))
    def _():
        signal(barrier, partner)

    def remote(src, dst, snd, rcv, peer):
        return pltpu.make_async_remote_copy(
            src_ref=src, dst_ref=dst, send_sem=snd, recv_sem=rcv,
            device_id={"seq": peer}, device_id_type=MESH,
        )

    mine = pl.ds(pl.multiple_of(core * tok, tok), tok)
    theirs = pl.ds(pl.multiple_of((1 - core) * tok, tok), tok)
    pairs_in = ((k_h, k_all), (v_h, v_all), (q_h, q_all), (g_h, g_all))

    def group(which, s):
        return col(which * heads + s, 1 if s < DELAY else heads - DELAY)

    def in_local(j, s):
        src, dst = pairs_in[j]
        return pltpu.make_async_copy(src.at[:, group(core, s)], dst.at[mine, group(0, s)], in_loc.at[j, s])

    def in_remote(j, s):
        src, dst = pairs_in[j]
        return remote(
            src.at[:, group(1 - core, s)], dst.at[mine, group(0, s)], in_snd.at[j, s], in_rcv.at[j, s], partner
        )

    seg_local = pltpu.make_async_copy(seg_h, seg_buf.at[0, core], seg_sem.at[0])
    seg_remote = remote(seg_h, seg_buf.at[0, core], seg_sem.at[1], seg_sem.at[2], partner)
    seg_right = remote(seg_buf.at[0], seg_buf.at[1], seg_sem.at[3], seg_sem.at[4], right)
    seg_left = remote(seg_buf.at[0], seg_buf.at[2], seg_sem.at[5], seg_sem.at[6], left)
    for s in range(DELAY + 1):
        for j in range(4):
            in_local(j, s).start()
    seg_local.start()
    pl.semaphore_wait(barrier, jnp.where(has_right, 3 - core, 1))

    @pl.when(has_right)
    def _():
        signal(ready.at[0], right)

    @pl.when(core == 0)
    def _():
        signal(ready.at[1], partner)

    head, below = pl.ds(0, span), pl.ds(2 * span, STAT)

    def early_left(t, i):
        src, dst = (
            (q_all.at[head, col(t)], rm.at[t, pl.ds(0, span)]),
            (g_all.at[head, col(t)], rm.at[t, pl.ds(span, span)]),
            (first.at[t], rm.at[t, below]),
        )[i]
        return remote(src, dst, e_snd.at[t, i], e_rcv.at[t, i], left)

    skip = own - span

    def early_right(t, i, source, target):
        count = tok - skip if source == 0 else tok
        at = i * span if source == 0 else i * span + tok - skip
        rows = pl.ds(skip, count) if source == 0 else pl.ds(0, count)
        return remote(
            pairs_in[i][0].at[rows, col(target * heads + t)], rp.at[t, pl.ds(at, count)],
            r_snd.at[t, i, target], r_rcv.at[t, i, source], 2 * lax.div(right, 2) + target,
        )

    def to_right(h):
        return remote(sendp.at[h], rp.at[h + DELAY], l_snd.at[0, h], l_rcv.at[0, h], right)

    def to_left(h):
        return remote(sendm.at[h], rm.at[h + DELAY], l_snd.at[1, h], l_rcv.at[1, h], left)

    for source in range(2):

        @pl.when(has_right & (core == source))
        def _():
            for t in range(DELAY):
                for target in range(2):
                    for i in range(2):
                        early_right(t, i, source, target).start()

    @pl.when(core == 1)
    def _():
        pl.semaphore_wait(ready.at[1], 1)

    seg_remote.start()
    for s in range(DELAY + 1):
        for j in range(4):
            in_remote(j, s).start()

    @pl.when(jnp.logical_not(has_left))
    def _():
        seg_buf[1] = jnp.full(seg_buf.shape[1:], -1, jnp.int32)

        def clear(t, _):
            rp[t] = jnp.zeros(rp.shape[1:], BF16)
            return 0

        lax.fori_loop(0, rp.shape[0], clear, 0)

    @pl.when(jnp.logical_not(has_right))
    def _():
        seg_buf[2] = jnp.full(seg_buf.shape[1:], -3, jnp.int32)

        def clear(t, _):
            rm[t] = jnp.zeros(rm.shape[1:], BF16)
            return 0

        lax.fori_loop(0, rm.shape[0], clear, 0)

    seg_local.wait()
    seg_remote.wait_recv()

    @pl.when(has_right)
    def _():
        seg_right.start()

    def rows(ref, h, at, blocks):
        parts = [ref[h, at + b : at + b + 1, :] for b in range(blocks)]
        return parts[0] if blocks == 1 else jnp.concatenate(parts, axis=1)

    def put_rows(ref, h, at, value):
        for b in range(value.shape[1] // hd):
            ref[h, at + b : at + b + 1, :] = value[:, b * hd : (b + 1) * hd]

    def encode(lse, delta):
        out = []
        for row in lse:
            top = row.astype(BF16).astype(F32)
            mid = (row - top).astype(BF16).astype(F32)
            out += [top, mid, row - top - mid]
        for row in delta:
            top = row.astype(BF16).astype(F32)
            out += [top, row - top]
        out.append(jnp.zeros_like(out[0]))
        return jnp.concatenate(out, axis=0).astype(BF16)

    def decode(ref, t):
        table = ref[t, 2 * span : 2 * span + STAT, :].astype(F32)
        lse = [table[3 * b : 3 * b + 1] + table[3 * b + 1 : 3 * b + 2] + table[3 * b + 2 : 3 * b + 3] for b in range(3)]
        delta = [table[9 + 2 * b : 10 + 2 * b] + table[10 + 2 * b : 11 + 2 * b] for b in range(3)]
        return lse, delta

    def own_stats(h):
        lses, deltas = [], []
        for b in range(2):
            depth = (b + 1) * wide
            at = slice(b * wide, (b + 1) * wide)
            s = dot_nt(k_all[:depth, col(h)], q_all[at, col(h)]) * scale + b_own[:depth, at]
            dp = dot_nt(v_all[:depth, col(h)], g_all[at, col(h)])
            m = colmax(s)
            p = jnp.exp2(s - m)
            total = colsum(p)
            lse, delta = m + jnp.log2(total), colsum(p * dp) / total
            put_rows(st_own, h, 2 * b, lse)
            put_rows(st_own, h, 4 + 2 * b, delta)
            lses += [lse[:, :hd], lse[:, hd:]]
            deltas += [delta[:, :hd], delta[:, hd:]]
        return encode(lses[:3], deltas[:3])

    def finish(s, dp, lse, delta):
        p = jnp.exp2(s - lse)
        return p.astype(BF16), (p * ((dp - delta) * inv_root)).astype(BF16)

    def merge(lse, delta, parts):
        m = lse
        for s, _ in parts:
            m = jnp.maximum(m, colmax(s))
        first = jnp.exp2(lse - m)
        total, dn = first, delta * first
        probs = []
        for s, dp in parts:
            p = jnp.exp2(s - m)
            total = total + colsum(p)
            dn = dn + colsum(p * dp)
            probs.append(p)
        inv = 1.0 / total
        delta = dn * inv
        outs = []
        for p, (_, dp) in zip(probs, parts):
            p = p * inv
            outs.append((p.astype(BF16), (p * ((dp - delta) * inv_root)).astype(BF16)))
        return m + jnp.log2(total), delta, outs

    def cross(h):
        cut = span - wide
        nxt = jnp.minimum(h + DELAY, heads - 1)
        fresh = jnp.where(h + DELAY < heads, 1.0, 0.0)
        keys_right = jnp.broadcast_to((1.0 - flags[1:2, :]) * fresh, (span, hd)) > 0.5
        queries_left = jnp.broadcast_to(flags[0:1, :] * fresh, (span, hd)) > 0.5
        kl, vl = rp[h, :span], rp[h, span : 2 * span]
        lse_in, delta_in = decode(rm, h)
        k, v = k_all[:, col(h)], v_all[:, col(h)]
        qa, ga = rm[h, :wide], rm[h, span : span + wide]
        s1 = dot_nt(k, qa) * scale + b_right[:, :wide]
        s2 = dot_nt(kl[cut:], qa) * scale + b_far[...]
        d1, d2 = dot_nt(v, ga), dot_nt(vl[cut:], ga)
        lse, delta, ((p1, e1), (p2, e2)) = merge(
            jnp.concatenate(lse_in[:2], 1), jnp.concatenate(delta_in[:2], 1), ((s1, d1), (s2, d2))
        )
        lse_out, delta_out = [lse[:, :hd], lse[:, hd:]], [delta[:, :hd], delta[:, hd:]]
        dk, dv = dot_nn(e1, qa), dot_nn(p1, ga)
        dkl, dvl = dot_nn(e2, qa), dot_nn(p2, ga)
        for i, (a1, b1, a2, b2, kept) in enumerate(
            ((p1, v, p2, vl[cut:], k_all), (e1, k, e2, kl[cut:], v_all))
        ):
            part = dot_tn(a1, b1) + dot_tn(a2, b2)
            stay = kept[own - span : own - span + wide, col(nxt)].astype(F32)
            sendp[h, i * span : i * span + wide] = jnp.where(keys_right[:wide], stay, part).astype(BF16)
        qb, gb = rm[h, wide:span], rm[h, span + wide : 2 * span]
        s3 = dot_nt(k, qb) * scale + b_right[:, wide:]
        d3 = dot_nt(v, gb)
        lse, delta, ((p3, e3),) = merge(lse_in[2], delta_in[2], ((s3, d3),))
        sendp[h, 2 * span :] = encode(lse_out + [lse], delta_out + [delta])
        acc_dk[h] = dk + dot_nn(e3, qb)
        acc_dv[h] = dv + dot_nn(p3, gb)
        for i, (a3, b3, kept) in enumerate(((p3, v, k_all), (e3, k, v_all))):
            part = dot_tn(a3, b3)
            stay = kept[own - span + wide :, col(nxt)].astype(F32)
            sendp[h, i * span + wide : (i + 1) * span] = jnp.where(keys_right[wide:], stay, part).astype(BF16)

        @pl.when(has_right)
        def _():
            to_right(h).start()

        dkl_sum = dvl_sum = None
        for b in range(2):
            at = slice(b * wide, (b + 1) * wide)
            q, g = q_all[at, col(h)], g_all[at, col(h)]
            s = dot_nt(kl, q) * scale + b_left[:, at]
            dp = dot_nt(vl, g)
            lse, delta, ((p, e),) = merge(
                rows(st_own, h, 2 * b, 2), rows(st_own, h, 4 + 2 * b, 2), ((s, dp),)
            )
            put_rows(st_tot, h, 2 * b, lse)
            put_rows(st_tot, h, 4 + 2 * b, delta)
            acc_o[h, at] = dot_tn(p, vl)
            acc_dq[h, at] = dot_tn(e, kl)
            dkb, dvb = dot_nn(e, q), dot_nn(p, g)
            dkl_sum = dkb if b == 0 else dkl_sum + dkb
            dvl_sum = dvb if b == 0 else dvl_sum + dvb
        for i, (total, extra, kept) in enumerate(((dkl_sum, dkl, q_all), (dvl_sum, dvl, g_all))):
            stay = kept[:span, col(nxt)].astype(F32)
            sendm[h, i * span : i * span + cut] = jnp.where(queries_left[:cut], stay[:cut], total[:cut]).astype(BF16)
            sendm[h, i * span + cut : (i + 1) * span] = jnp.where(
                queries_left[cut:], stay[cut:], total[cut:] + extra
            ).astype(BF16)

    def close(h):
        t = h + DELAY
        asked = flags[0:1, :] > 0.5
        back = jnp.broadcast_to(flags[0:1, :], (span, hd)) > 0.5
        back_keys = jnp.broadcast_to(1.0 - flags[1:2, :], (span, hd)) > 0.5
        lse = [st_tot[h, b : b + 1, :] for b in range(4)]
        delta = [st_tot[h, 4 + b : 5 + b, :] for b in range(4)]
        lse_back, delta_back = decode(rp, t)
        for b in range(3):
            lse[b] = jnp.where(asked, lse_back[b], lse[b])
            delta[b] = jnp.where(asked, delta_back[b], delta[b])
        add = [jnp.where(back, rp[t, i * span : (i + 1) * span].astype(F32), 0.0) for i in range(2)]
        for b in range(2):
            depth = (b + 1) * wide
            at = slice(b * wide, (b + 1) * wide)
            q, g = q_all[at, col(h)], g_all[at, col(h)]
            k, v = k_all[:depth, col(h)], v_all[:depth, col(h)]
            s = dot_nt(k, q) * scale + b_own[:depth, at]
            dp = dot_nt(v, g)
            p, e = finish(
                s, dp, jnp.concatenate(lse[2 * b : 2 * b + 2], 1), jnp.concatenate(delta[2 * b : 2 * b + 2], 1)
            )
            acc_dk[h, :depth] += dot_nn(e, q)
            acc_dv[h, :depth] += dot_nn(p, g)
            for i, (value, acc) in enumerate(((dot_tn(p, v), acc_o), (dot_tn(e, k), acc_dq))):
                value = value + acc[h, at]
                if b == 0:
                    staged[h, i, at] = (value + add[i][:wide]).astype(BF16)
                else:
                    staged[h, i, wide:span] = (value[: span - wide] + add[i][wide:]).astype(BF16)
                    staged[h, i, span:] = value[span - wide :].astype(BF16)
        for i, acc in ((0, acc_dk), (1, acc_dv)):
            staged[h, 2 + i, : own - span] = acc[h, : own - span].astype(BF16)
            staged[h, 2 + i, own - span :] = (
                acc[h, own - span :] + jnp.where(back_keys, rm[t, i * span : (i + 1) * span].astype(F32), 0.0)
            ).astype(BF16)

    outs = (o_h, dq_h, dk_h, dv_h)

    def out_remote(j, h):
        return remote(
            staged.at[h, j, theirs], outs[j].at[:, col(core * heads + h)],
            out_snd.at[j, h], out_rcv.at[j, h], partner,
        )

    def seg_row(chip, b):
        return seg_buf[chip, b // 2, b % 2 : b % 2 + 1, :].astype(F32)

    def as_column(row):
        return jnp.transpose(jnp.broadcast_to(row, (hd, hd)))

    def tile(a, b):
        return slice(a * hd, (a + 1) * hd), slice(b * hd, (b + 1) * hd)

    own_rows = [seg_row(0, b) for b in range(4)]
    own_cols = [as_column(row) for row in own_rows]
    causal = lax.broadcasted_iota(jnp.int32, (hd, hd), 0) <= lax.broadcasted_iota(jnp.int32, (hd, hd), 1)
    for a in range(4):
        for b in range(4):
            same = own_cols[a] == own_rows[b]
            if a > b:
                b_own[tile(a, b)] = jnp.full((hd, hd), NEG, F32)
            else:
                b_own[tile(a, b)] = jnp.where(same & causal if a == b else same, 0.0, NEG)

    for t in range(DELAY):
        for j in range(4):
            in_local(j, t).wait()
            in_remote(j, t).wait_recv()
        first[t] = own_stats(t)

    @pl.when(has_left)
    def _():
        pl.semaphore_wait(ready.at[0], 1)
        for t in range(DELAY):
            for i in range(3):
                early_left(t, i).start()
            if t == 0:
                seg_left.start()
        seg_right.wait_recv()

    @pl.when(has_right)
    def _():
        seg_left.wait_recv()

    def seg_at(chip, b, lane):
        return jnp.broadcast_to(seg_row(chip, b)[:, lane : lane + 1], (1, hd))

    asks_left = seg_at(1, 0, hd - 1) == seg_at(0, 0, 0)
    asks_right = seg_at(0, 0, hd - 1) == seg_at(2, 0, 0)
    flags[0:1, :] = jnp.where(asks_left, 1.0, 0.0)
    flags[1:2, :] = jnp.where(asks_right, 1.0, 0.0)
    left_cols = [as_column(jnp.where(asks_left, -1.0, seg_row(1, b + 1))) for b in range(3)]
    right_rows = [jnp.where(asks_right, seg_row(2, b), -2.0) for b in range(3)]
    for a in range(4):
        for b in range(4):
            if a < 3:
                b_left[tile(a, b)] = jnp.where(left_cols[a] == own_rows[b], 0.0, NEG)
            if b < 3:
                b_right[tile(a, b)] = jnp.where(own_cols[a] == right_rows[b], 0.0, NEG)
            if a < 2 and b < 2:
                b_far[tile(a, b)] = jnp.where(left_cols[a + 1] == right_rows[b], 0.0, NEG)

    def step(i, _):
        @pl.when(i == 0)
        def _():
            for j in range(4):
                in_local(j, DELAY).wait()
                in_remote(j, DELAY).wait_recv()

        @pl.when(i + DELAY < heads)
        def _():
            sendm[i, 2 * span :] = own_stats(i + DELAY)

        @pl.when(i >= heads - DELAY)
        def _():
            @pl.when(i < heads)
            def _():
                sendm[i, 2 * span :] = jnp.zeros((STAT, hd), BF16)

        @pl.when((i < DELAY) & has_left)
        def _():
            for j in range(2):
                for source in range(2):
                    early_right(i, j, source, 0).wait_recv()
            for j in range(3):
                early_left(i, j).wait_send()

        @pl.when((i < DELAY) & has_right)
        def _():
            for j in range(3):
                early_left(i, j).wait_recv()

        @pl.when((i >= DELAY) & has_left)
        def _():
            to_right(i - DELAY).wait_recv()
            to_left(i - DELAY).wait_send()

        @pl.when((i >= DELAY) & has_right)
        def _():
            to_left(i - DELAY).wait_recv()
            to_right(i - DELAY).wait_send()

        @pl.when(i < heads)
        def _():
            cross(i)

            @pl.when(has_left)
            def _():
                to_left(i).start()

        @pl.when(i >= DELAY)
        def _():
            h = i - DELAY
            close(h)
            for j in range(4):
                out_remote(j, h).start()
            for j in range(4):
                outs[j][:, col(core * heads + h)] = staged[h, j, mine, :]

        @pl.when(i > DELAY)
        def _():
            for j in range(4):
                out_remote(j, i - DELAY - 1).wait()

        return 0

    lax.fori_loop(0, heads + DELAY, step, 0)
    for s in range(DELAY + 1):
        for j in range(4):
            in_remote(j, s).wait_send()
    for j in range(4):
        out_remote(j, heads - 1).wait()
    seg_remote.wait_send()

    for source in range(2):

        @pl.when(has_right & (core == source))
        def _():
            for t in range(DELAY):
                for target in range(2):
                    for i in range(2):
                        early_right(t, i, source, target).wait_send()

    @pl.when(has_right)
    def _():
        seg_right.wait_send()

    @pl.when(has_left)
    def _():
        seg_left.wait_send()


def store(*refs):
    sem = refs[8]
    copies = [pltpu.make_async_copy(refs[j], refs[4 + j], sem.at[j]) for j in range(4)]
    for copy in copies:
        copy.start()
    for copy in copies:
        copy.wait()


def local(n, queries, keys, values, out_grad, segments):
    tok, feature = queries.shape
    heads, hd = HEADS // 2, feature // HEADS
    own = 2 * tok
    span = own - hd
    slots = heads + DELAY
    rows = 2 * span + STAT
    out = jax.ShapeDtypeStruct((tok, feature), BF16)
    dma = pltpu.SemaphoreType.DMA
    vm = pltpu.VMEM
    results = pl.pallas_call(
        functools.partial(kernel, n),
        out_shape=(vm((tok, feature), BF16),) * 4,
        in_specs=[pl.BlockSpec(memory_space=pltpu.HBM)] * 5,
        out_specs=[pl.BlockSpec(memory_space=vm)] * 4,
        scratch_shapes=[
            vm((own, heads * hd), BF16), vm((own, heads * hd), BF16),
            vm((own, heads * hd), BF16), vm((own, heads * hd), BF16),
            vm((3, 2, 2, hd), jnp.int32), vm((8, hd), F32),
            vm((own, own), F32), vm((span, own), F32), vm((own, span), F32), vm((2 * hd, 2 * hd), F32),
            vm((slots, rows, hd), BF16), vm((slots, rows, hd), BF16),
            vm((heads, rows, hd), BF16), vm((heads, rows, hd), BF16), vm((DELAY, STAT, hd), BF16),
            vm((heads, 8, hd), F32), vm((heads, 8, hd), F32),
            vm((heads, own, hd), F32), vm((heads, own, hd), F32),
            vm((heads, own, hd), F32), vm((heads, own, hd), F32),
            vm((heads, 4, own, hd), BF16),
            dma((4, DELAY + 1)), dma((4, DELAY + 1)), dma((4, DELAY + 1)), dma((7,)),
            dma((DELAY, 2, 2)), dma((DELAY, 2, 2)), dma((DELAY, 3)), dma((DELAY, 3)),
            dma((2, heads)), dma((2, heads)), pltpu.SemaphoreType.REGULAR((2,)),
            dma((4, heads)), dma((4, heads)),
        ],
        compiler_params=pltpu.CompilerParams(
            collective_id=0, has_side_effects=True, vmem_limit_bytes=51 * 2**20
        ),
        name="packed_attention",
    )(*(pltpu.with_memory_space_constraint(x, pltpu.HBM) for x in (queries, keys, values, out_grad)), segments.reshape(2, tok // 2))
    return pl.pallas_call(
        store,
        out_shape=(out,) * 4,
        in_specs=[pl.BlockSpec(memory_space=pl.ANY)] * 4,
        out_specs=[pl.BlockSpec(memory_space=pl.ANY)] * 4,
        scratch_shapes=[dma((4,))],
        compiler_params=pltpu.CompilerParams(vmem_limit_bytes=2**20),
        name="store_results",
    )(*(pltpu.with_memory_space_constraint(r, vm) for r in results))


def solution(mesh):
    spec = P(("branch", "seq"), None)
    return jax.shard_map(
        functools.partial(local, mesh.shape["seq"]),
        mesh=mesh,
        in_specs=(spec,) * 4 + (P(("branch", "seq")),),
        out_specs=(spec,) * 4,
        check_vma=False,
    )
```

```python
import functools
import math

import jax
import jax.numpy as jnp
from jax import lax
from jax.experimental import pallas as pl
from jax.experimental.pallas import tpu as pltpu
from jax.sharding import PartitionSpec as P

HEADS = 16
MESH = pl.DeviceIdType.MESH
DELAY = 2
NEG = -1e30
STAT = 16
F32 = jnp.float32
BF16 = jnp.bfloat16


def dot_nt(a, b):
    return lax.dot_general(a, b, (((1,), (1,)), ((), ())), preferred_element_type=F32)


def dot_nn(a, b):
    return lax.dot_general(a, b, (((1,), (0,)), ((), ())), preferred_element_type=F32)


def dot_tn(a, b):
    return lax.dot_general(a, b, (((0,), (0,)), ((), ())), preferred_element_type=F32)


def colsum(x):
    return jnp.sum(x, axis=0, keepdims=True)


def colmax(x):
    return jnp.max(x, axis=0, keepdims=True)


def kernel(
    n,
    q_h, k_h, v_h, g_h, seg_h,
    o_h, dq_h, dk_h, dv_h,
    q_all, k_all, v_all, g_all, seg_buf, flags,
    b_own, b_left, b_right, b_far,
    rp, rm, sendp, sendm, first,
    st_own, st_tot, st_max, probs, dprobs,
    acc_o, acc_dq, acc_dk, acc_dv, staged,
    in_loc, in_snd, in_rcv, seg_sem,
    r_snd, r_rcv, e_snd, e_rcv, l_snd, l_rcv, ready,
    out_snd, out_rcv,
):
    tok, feature = q_h.shape
    heads = HEADS // 2
    hd = feature // HEADS
    own = 2 * tok
    span = own - hd
    scale = math.log2(math.e) / math.sqrt(hd)
    inv_root = 1.0 / math.sqrt(hd)
    wide = 2 * hd

    def col(h, count=1):
        start = h * hd if isinstance(h, int) else pl.multiple_of(h * hd, hd)
        return pl.ds(start, count * hd)

    me = lax.axis_index("seq")
    core = lax.rem(me, 2)
    partner = me + 1 - 2 * core
    chip = lax.div(me, 2)
    left = lax.rem(me + n - 2, n)
    right = lax.rem(me + 2, n)
    has_left = chip > 0
    has_right = chip < n // 2 - 1

    barrier = pltpu.get_barrier_semaphore()

    def signal(sem, peer):
        pl.semaphore_signal(sem, inc=1, device_id={"seq": peer}, device_id_type=MESH)

    @pl.when(has_left)
    def _():
        for c in range(2):
            signal(barrier, 2 * lax.div(left, 2) + c)

    @pl.when((core == 1) | jnp.logical_not(has_right))
    def _():
        signal(barrier, partner)

    def remote(src, dst, snd, rcv, peer):
        return pltpu.make_async_remote_copy(
            src_ref=src, dst_ref=dst, send_sem=snd, recv_sem=rcv,
            device_id={"seq": peer}, device_id_type=MESH,
        )

    mine = pl.ds(pl.multiple_of(core * tok, tok), tok)
    theirs = pl.ds(pl.multiple_of((1 - core) * tok, tok), tok)
    pairs_in = ((k_h, k_all), (v_h, v_all), (q_h, q_all), (g_h, g_all))

    def group(which, s):
        return col(which * heads + s, 1 if s < DELAY else heads - DELAY)

    def in_local(j, s):
        src, dst = pairs_in[j]
        return pltpu.make_async_copy(src.at[:, group(core, s)], dst.at[mine, group(0, s)], in_loc.at[j, s])

    def in_remote(j, s):
        src, dst = pairs_in[j]
        return remote(
            src.at[:, group(1 - core, s)], dst.at[mine, group(0, s)], in_snd.at[j, s], in_rcv.at[j, s], partner
        )

    seg_local = pltpu.make_async_copy(seg_h, seg_buf.at[0, core], seg_sem.at[0])
    seg_remote = remote(seg_h, seg_buf.at[0, core], seg_sem.at[1], seg_sem.at[2], partner)
    seg_right = remote(seg_buf.at[0], seg_buf.at[1], seg_sem.at[3], seg_sem.at[4], right)
    seg_left = remote(seg_buf.at[0], seg_buf.at[2], seg_sem.at[5], seg_sem.at[6], left)
    pl.semaphore_wait(barrier, jnp.where(has_right, 3 - core, 1))

    @pl.when(has_right)
    def _():
        signal(ready.at[0], right)

    @pl.when(core == 0)
    def _():
        signal(ready.at[1], partner)

    head, below = pl.ds(0, span), pl.ds(2 * span, STAT)

    def early_left(t, i):
        src, dst = (
            (q_all.at[head, col(t)], rm.at[t, pl.ds(0, span)]),
            (g_all.at[head, col(t)], rm.at[t, pl.ds(span, span)]),
            (first.at[t], rm.at[t, below]),
        )[i]
        return remote(src, dst, e_snd.at[t, i], e_rcv.at[t, i], left)

    skip = own - span

    def early_right(t, i, source, target):
        count = tok - skip if source == 0 else tok
        at = i * span if source == 0 else i * span + tok - skip
        rows = pl.ds(skip, count) if source == 0 else pl.ds(0, count)
        return remote(
            pairs_in[i][0].at[rows, col(target * heads + t)], rp.at[t, pl.ds(at, count)],
            r_snd.at[t, i, target], r_rcv.at[t, i, source], 2 * lax.div(right, 2) + target,
        )

    def to_right(h):
        return remote(sendp.at[h], rp.at[h + DELAY], l_snd.at[0, h], l_rcv.at[0, h], right)

    def to_left(h):
        return remote(sendm.at[h], rm.at[h + DELAY], l_snd.at[1, h], l_rcv.at[1, h], left)

    for source in range(2):

        @pl.when(has_right & (core == source))
        def _():
            for t in range(DELAY):
                for target in range(2):
                    for i in range(2):
                        early_right(t, i, source, target).start()

    @pl.when(core == 1)
    def _():
        pl.semaphore_wait(ready.at[1], 1)

    seg_remote.start()
    seg_local.start()
    for s in range(DELAY + 1):
        for j in range(4):
            in_remote(j, s).start()
            in_local(j, s).start()

    @pl.when(jnp.logical_not(has_left))
    def _():
        seg_buf[1] = jnp.full(seg_buf.shape[1:], -1, jnp.int32)

        def clear(t, _):
            rp[t] = jnp.zeros(rp.shape[1:], BF16)
            return 0

        lax.fori_loop(0, rp.shape[0], clear, 0)

    @pl.when(jnp.logical_not(has_right))
    def _():
        seg_buf[2] = jnp.full(seg_buf.shape[1:], -3, jnp.int32)

        def clear(t, _):
            rm[t] = jnp.zeros(rm.shape[1:], BF16)
            return 0

        lax.fori_loop(0, rm.shape[0], clear, 0)

    seg_local.wait()
    seg_remote.wait_recv()

    @pl.when(has_right)
    def _():
        seg_right.start()

    def rows(ref, h, at, blocks):
        parts = [ref[h, at + b : at + b + 1, :] for b in range(blocks)]
        return parts[0] if blocks == 1 else jnp.concatenate(parts, axis=1)

    def put_rows(ref, h, at, value):
        for b in range(value.shape[1] // hd):
            ref[h, at + b : at + b + 1, :] = value[:, b * hd : (b + 1) * hd]

    def encode(lse, delta):
        out = []
        for row in lse:
            top = row.astype(BF16).astype(F32)
            mid = (row - top).astype(BF16).astype(F32)
            out += [top, mid, row - top - mid]
        for row in delta:
            top = row.astype(BF16).astype(F32)
            out += [top, row - top]
        out.append(jnp.zeros_like(out[0]))
        return jnp.concatenate(out, axis=0).astype(BF16)

    def decode(ref, t):
        table = ref[t, 2 * span : 2 * span + STAT, :].astype(F32)
        lse = [table[3 * b : 3 * b + 1] + table[3 * b + 1 : 3 * b + 2] + table[3 * b + 2 : 3 * b + 3] for b in range(3)]
        delta = [table[9 + 2 * b : 10 + 2 * b] + table[10 + 2 * b : 11 + 2 * b] for b in range(3)]
        return lse, delta

    def own_stats(h):
        lses, deltas = [], []
        for b in range(2):
            depth = (b + 1) * wide
            at = slice(b * wide, (b + 1) * wide)
            s = dot_nt(k_all[:depth, col(h)], q_all[at, col(h)]) * scale + b_own[:depth, at]
            dp = dot_nt(v_all[:depth, col(h)], g_all[at, col(h)])
            m = colmax(s)
            p = jnp.exp2(s - m)
            total = colsum(p)
            kept = slice(b * wide, b * wide + depth)
            probs[h, kept], dprobs[h, kept] = p, dp
            put_rows(st_max, h, 2 * b, m)
            lse, delta = m + jnp.log2(total), colsum(p * dp) / total
            put_rows(st_own, h, 2 * b, lse)
            put_rows(st_own, h, 4 + 2 * b, delta)
            lses += [lse[:, :hd], lse[:, hd:]]
            deltas += [delta[:, :hd], delta[:, hd:]]
        return encode(lses[:3], deltas[:3])

    def merge(lse, delta, parts):
        m = lse
        for s, _ in parts:
            m = jnp.maximum(m, colmax(s))
        first = jnp.exp2(lse - m)
        total, dn = first, delta * first
        probs = []
        for s, dp in parts:
            p = jnp.exp2(s - m)
            total = total + colsum(p)
            dn = dn + colsum(p * dp)
            probs.append(p)
        inv = 1.0 / total
        delta = dn * inv
        outs = []
        for p, (_, dp) in zip(probs, parts):
            p = p * inv
            outs.append((p.astype(BF16), (p * ((dp - delta) * inv_root)).astype(BF16)))
        return m + jnp.log2(total), delta, outs

    def cross(h):
        cut = span - wide
        nxt = jnp.minimum(h + DELAY, heads - 1)
        fresh = jnp.where(h + DELAY < heads, 1.0, 0.0)
        keys_right = jnp.broadcast_to((1.0 - flags[1:2, :]) * fresh, (span, hd)) > 0.5
        queries_left = jnp.broadcast_to(flags[0:1, :] * fresh, (span, hd)) > 0.5
        kl, vl = rp[h, :span], rp[h, span : 2 * span]
        lse_in, delta_in = decode(rm, h)
        k, v = k_all[:, col(h)], v_all[:, col(h)]
        qa, ga = rm[h, :wide], rm[h, span : span + wide]
        s1 = dot_nt(k, qa) * scale + b_right[:, :wide]
        s2 = dot_nt(kl[cut:], qa) * scale + b_far[...]
        d1, d2 = dot_nt(v, ga), dot_nt(vl[cut:], ga)
        lse, delta, ((p1, e1), (p2, e2)) = merge(
            jnp.concatenate(lse_in[:2], 1), jnp.concatenate(delta_in[:2], 1), ((s1, d1), (s2, d2))
        )
        lse_out, delta_out = [lse[:, :hd], lse[:, hd:]], [delta[:, :hd], delta[:, hd:]]
        for i, (a1, b1, a2, b2, kept) in enumerate(
            ((p1, v, p2, vl[cut:], k_all), (e1, k, e2, kl[cut:], v_all))
        ):
            part = dot_tn(a1, b1) + dot_tn(a2, b2)
            stay = kept[own - span : own - span + wide, col(nxt)].astype(F32)
            sendp[h, i * span : i * span + wide] = jnp.where(keys_right[:wide], stay, part).astype(BF16)
        qb, gb = rm[h, wide:span], rm[h, span + wide : 2 * span]
        s3 = dot_nt(k, qb) * scale + b_right[:, wide:]
        d3 = dot_nt(v, gb)
        lse, delta, ((p3, e3),) = merge(lse_in[2], delta_in[2], ((s3, d3),))
        sendp[h, 2 * span :] = encode(lse_out + [lse], delta_out + [delta])
        for i, (a3, b3, kept) in enumerate(((p3, v, k_all), (e3, k, v_all))):
            part = dot_tn(a3, b3)
            stay = kept[own - span + wide :, col(nxt)].astype(F32)
            sendp[h, i * span + wide : (i + 1) * span] = jnp.where(keys_right[wide:], stay, part).astype(BF16)

        @pl.when(has_right)
        def _():
            to_right(h).start()

        dkl_sum = dvl_sum = None
        dkl, dvl = dot_nn(e2, qa), dot_nn(p2, ga)
        stay_here = []
        for b in range(2):
            at = slice(b * wide, (b + 1) * wide)
            q, g = q_all[at, col(h)], g_all[at, col(h)]
            s = dot_nt(kl, q) * scale + b_left[:, at]
            dp = dot_nt(vl, g)
            lse, delta, ((p, e),) = merge(
                rows(st_own, h, 2 * b, 2), rows(st_own, h, 4 + 2 * b, 2), ((s, dp),)
            )
            put_rows(st_tot, h, 2 * b, lse)
            put_rows(st_tot, h, 4 + 2 * b, delta)
            stay_here.append((at, p, e))
            dkb, dvb = dot_nn(e, q), dot_nn(p, g)
            dkl_sum = dkb if b == 0 else dkl_sum + dkb
            dvl_sum = dvb if b == 0 else dvl_sum + dvb
        for i, (total, extra, kept) in enumerate(((dkl_sum, dkl, q_all), (dvl_sum, dvl, g_all))):
            stay = kept[:span, col(nxt)].astype(F32)
            sendm[h, i * span : i * span + cut] = jnp.where(queries_left[:cut], stay[:cut], total[:cut]).astype(BF16)
            sendm[h, i * span + cut : (i + 1) * span] = jnp.where(
                queries_left[cut:], stay[cut:], total[cut:] + extra
            ).astype(BF16)

        @pl.when(has_left)
        def _():
            to_left(h).start()

        acc_dk[h] = dot_nn(e1, qa) + dot_nn(e3, qb)
        acc_dv[h] = dot_nn(p1, ga) + dot_nn(p3, gb)
        for at, p, e in stay_here:
            acc_o[h, at] = dot_tn(p, vl)
            acc_dq[h, at] = dot_tn(e, kl)

    def close(h):
        t = h + DELAY
        asked = flags[0:1, :] > 0.5
        back = jnp.broadcast_to(flags[0:1, :], (span, hd)) > 0.5
        back_keys = jnp.broadcast_to(1.0 - flags[1:2, :], (span, hd)) > 0.5
        lse = [st_tot[h, b : b + 1, :] for b in range(4)]
        delta = [st_tot[h, 4 + b : 5 + b, :] for b in range(4)]
        lse_back, delta_back = decode(rp, t)
        for b in range(3):
            lse[b] = jnp.where(asked, lse_back[b], lse[b])
            delta[b] = jnp.where(asked, delta_back[b], delta[b])
        add = [jnp.where(back, rp[t, i * span : (i + 1) * span].astype(F32), 0.0) for i in range(2)]
        for b in range(2):
            depth = (b + 1) * wide
            at = slice(b * wide, (b + 1) * wide)
            q, g = q_all[at, col(h)], g_all[at, col(h)]
            k, v = k_all[:depth, col(h)], v_all[:depth, col(h)]
            kept = slice(b * wide, b * wide + depth)
            shrink = jnp.exp2(rows(st_max, h, 2 * b, 2) - jnp.concatenate(lse[2 * b : 2 * b + 2], 1))
            p = probs[h, kept] * shrink
            e = (p * ((dprobs[h, kept] - jnp.concatenate(delta[2 * b : 2 * b + 2], 1)) * inv_root)).astype(BF16)
            p = p.astype(BF16)
            acc_dk[h, :depth] += dot_nn(e, q)
            acc_dv[h, :depth] += dot_nn(p, g)
            for i, (value, acc) in enumerate(((dot_tn(p, v), acc_o), (dot_tn(e, k), acc_dq))):
                value = value + acc[h, at]
                if b == 0:
                    staged[h, i, at] = (value + add[i][:wide]).astype(BF16)
                else:
                    staged[h, i, wide:span] = (value[: span - wide] + add[i][wide:]).astype(BF16)
                    staged[h, i, span:] = value[span - wide :].astype(BF16)
        for j in range(2):
            out_remote(j, h).start()
        for i, acc in ((0, acc_dk), (1, acc_dv)):
            staged[h, 2 + i, : own - span] = acc[h, : own - span].astype(BF16)
            staged[h, 2 + i, own - span :] = (
                acc[h, own - span :] + jnp.where(back_keys, rm[t, i * span : (i + 1) * span].astype(F32), 0.0)
            ).astype(BF16)

    outs = (o_h, dq_h, dk_h, dv_h)

    def out_remote(j, h):
        return remote(
            staged.at[h, j, theirs], outs[j].at[:, col(core * heads + h)],
            out_snd.at[j, h], out_rcv.at[j, h], partner,
        )

    def seg_row(chip, b):
        return seg_buf[chip, b // 2, b % 2 : b % 2 + 1, :].astype(F32)

    def as_column(row):
        return jnp.transpose(jnp.broadcast_to(row, (hd, hd)))

    def tile(a, b):
        return slice(a * hd, (a + 1) * hd), slice(b * hd, (b + 1) * hd)

    own_rows = [seg_row(0, b) for b in range(4)]
    own_cols = [as_column(row) for row in own_rows]
    causal = lax.broadcasted_iota(jnp.int32, (hd, hd), 0) <= lax.broadcasted_iota(jnp.int32, (hd, hd), 1)
    for a in range(4):
        for b in range(4):
            same = own_cols[a] == own_rows[b]
            if a > b:
                b_own[tile(a, b)] = jnp.full((hd, hd), NEG, F32)
            else:
                b_own[tile(a, b)] = jnp.where(same & causal if a == b else same, 0.0, NEG)

    for t in range(DELAY):
        for j in range(4):
            in_local(j, t).wait()
            in_remote(j, t).wait_recv()
        first[t] = own_stats(t)

    @pl.when(has_left)
    def _():
        pl.semaphore_wait(ready.at[0], 1)
        for t in range(DELAY):
            for i in range(3):
                early_left(t, i).start()
            if t == 0:
                seg_left.start()
        seg_right.wait_recv()

    @pl.when(has_right)
    def _():
        seg_left.wait_recv()

    def seg_at(chip, b, lane):
        return jnp.broadcast_to(seg_row(chip, b)[:, lane : lane + 1], (1, hd))

    asks_left = seg_at(1, 0, hd - 1) == seg_at(0, 0, 0)
    asks_right = seg_at(0, 0, hd - 1) == seg_at(2, 0, 0)
    flags[0:1, :] = jnp.where(asks_left, 1.0, 0.0)
    flags[1:2, :] = jnp.where(asks_right, 1.0, 0.0)
    left_cols = [as_column(jnp.where(asks_left, -1.0, seg_row(1, b + 1))) for b in range(3)]
    right_rows = [jnp.where(asks_right, seg_row(2, b), -2.0) for b in range(3)]
    for a in range(4):
        for b in range(4):
            if a < 3:
                b_left[tile(a, b)] = jnp.where(left_cols[a] == own_rows[b], 0.0, NEG)
            if b < 3:
                b_right[tile(a, b)] = jnp.where(own_cols[a] == right_rows[b], 0.0, NEG)
            if a < 2 and b < 2:
                b_far[tile(a, b)] = jnp.where(left_cols[a + 1] == right_rows[b], 0.0, NEG)

    def step(i, _):
        @pl.when(i == 0)
        def _():
            for j in range(4):
                in_local(j, DELAY).wait()
                in_remote(j, DELAY).wait_recv()

        @pl.when(i + DELAY < heads)
        def _():
            sendm[i, 2 * span :] = own_stats(i + DELAY)

        @pl.when(i >= heads - DELAY)
        def _():
            @pl.when(i < heads)
            def _():
                sendm[i, 2 * span :] = jnp.zeros((STAT, hd), BF16)

        @pl.when((i < DELAY) & has_left)
        def _():
            for j in range(2):
                for source in range(2):
                    early_right(i, j, source, 0).wait_recv()
            for j in range(3):
                early_left(i, j).wait_send()

        @pl.when((i < DELAY) & has_right)
        def _():
            for j in range(3):
                early_left(i, j).wait_recv()

        @pl.when((i >= DELAY) & has_left)
        def _():
            to_right(i - DELAY).wait_recv()
            to_left(i - DELAY).wait_send()

        @pl.when((i >= DELAY) & has_right)
        def _():
            to_left(i - DELAY).wait_recv()
            to_right(i - DELAY).wait_send()

        @pl.when(i < heads)
        def _():
            cross(i)

        @pl.when(i >= DELAY)
        def _():
            h = i - DELAY
            close(h)
            for j in range(2, 4):
                out_remote(j, h).start()
            for j in range(4):
                outs[j][:, col(core * heads + h)] = staged[h, j, mine, :]

        @pl.when(i > DELAY)
        def _():
            for j in range(4):
                out_remote(j, i - DELAY - 1).wait()

        return 0

    lax.fori_loop(0, heads + DELAY, step, 0)
    for s in range(DELAY + 1):
        for j in range(4):
            in_remote(j, s).wait_send()
    for j in range(4):
        out_remote(j, heads - 1).wait()
    seg_remote.wait_send()

    for source in range(2):

        @pl.when(has_right & (core == source))
        def _():
            for t in range(DELAY):
                for target in range(2):
                    for i in range(2):
                        early_right(t, i, source, target).wait_send()

    @pl.when(has_right)
    def _():
        seg_right.wait_send()

    @pl.when(has_left)
    def _():
        seg_left.wait_send()


def store(*refs):
    sem = refs[8]
    copies = [pltpu.make_async_copy(refs[j], refs[4 + j], sem.at[j]) for j in range(4)]
    for copy in copies:
        copy.start()
    for copy in copies:
        copy.wait()


def local(n, queries, keys, values, out_grad, segments):
    tok, feature = queries.shape
    heads, hd = HEADS // 2, feature // HEADS
    own = 2 * tok
    span = own - hd
    slots = heads + DELAY
    rows = 2 * span + STAT
    out = jax.ShapeDtypeStruct((tok, feature), BF16)
    dma = pltpu.SemaphoreType.DMA
    vm = pltpu.VMEM
    results = pl.pallas_call(
        functools.partial(kernel, n),
        out_shape=(vm((tok, feature), BF16),) * 4,
        in_specs=[pl.BlockSpec(memory_space=pltpu.HBM)] * 5,
        out_specs=[pl.BlockSpec(memory_space=vm)] * 4,
        scratch_shapes=[
            vm((own, heads * hd), BF16), vm((own, heads * hd), BF16),
            vm((own, heads * hd), BF16), vm((own, heads * hd), BF16),
            vm((3, 2, 2, hd), jnp.int32), vm((8, hd), F32),
            vm((own, own), F32), vm((span, own), F32), vm((own, span), F32), vm((2 * hd, 2 * hd), F32),
            vm((slots, rows, hd), BF16), vm((slots, rows, hd), BF16),
            vm((heads, rows, hd), BF16), vm((heads, rows, hd), BF16), vm((DELAY, STAT, hd), BF16),
            vm((heads, 8, hd), F32), vm((heads, 8, hd), F32), vm((heads, 8, hd), F32),
            vm((heads, 6 * hd, 2 * hd), F32), vm((heads, 6 * hd, 2 * hd), F32),
            vm((heads, own, hd), F32), vm((heads, own, hd), F32),
            vm((heads, own, hd), F32), vm((heads, own, hd), F32),
            vm((heads, 4, own, hd), BF16),
            dma((4, DELAY + 1)), dma((4, DELAY + 1)), dma((4, DELAY + 1)), dma((7,)),
            dma((DELAY, 2, 2)), dma((DELAY, 2, 2)), dma((DELAY, 3)), dma((DELAY, 3)),
            dma((2, heads)), dma((2, heads)), pltpu.SemaphoreType.REGULAR((2,)),
            dma((4, heads)), dma((4, heads)),
        ],
        compiler_params=pltpu.CompilerParams(
            collective_id=0, has_side_effects=True, vmem_limit_bytes=51 * 2**20
        ),
        name="packed_attention",
    )(*(pltpu.with_memory_space_constraint(x, pltpu.HBM) for x in (queries, keys, values, out_grad)), segments.reshape(2, tok // 2))
    return pl.pallas_call(
        store,
        out_shape=(out,) * 4,
        in_specs=[pl.BlockSpec(memory_space=pl.ANY)] * 4,
        out_specs=[pl.BlockSpec(memory_space=pl.ANY)] * 4,
        scratch_shapes=[dma((4,))],
        compiler_params=pltpu.CompilerParams(vmem_limit_bytes=2**20),
        name="store_results",
    )(*(pltpu.with_memory_space_constraint(r, vm) for r in results))


def solution(mesh):
    spec = P(("branch", "seq"), None)
    return jax.shard_map(
        functools.partial(local, mesh.shape["seq"]),
        mesh=mesh,
        in_specs=(spec,) * 4 + (P(("branch", "seq")),),
        out_specs=(spec,) * 4,
        check_vma=False,
    )
```

```python
import functools
import math

import jax
import jax.numpy as jnp
from jax import lax
from jax.experimental import pallas as pl
from jax.experimental.pallas import tpu as pltpu
from jax.sharding import PartitionSpec as P

HEADS = 16
MESH = pl.DeviceIdType.MESH
DELAY = 2
NEG = -1e30
STAT = 16
F32 = jnp.float32
BF16 = jnp.bfloat16


def dot_nt(a, b):
    return lax.dot_general(a, b, (((1,), (1,)), ((), ())), preferred_element_type=F32)


def dot_nn(a, b):
    return lax.dot_general(a, b, (((1,), (0,)), ((), ())), preferred_element_type=F32)


def dot_tn(a, b):
    return lax.dot_general(a, b, (((0,), (0,)), ((), ())), preferred_element_type=F32)


def colsum(x):
    return jnp.sum(x, axis=0, keepdims=True)


def colmax(x):
    return jnp.max(x, axis=0, keepdims=True)


def kernel(
    n,
    q_h, k_h, v_h, g_h, seg_h,
    o_h, dq_h, dk_h, dv_h,
    q_all, k_all, v_all, g_all, seg_buf, flags,
    b_own, b_left, b_right, b_far,
    rp, rm, sendp, sendm, first,
    st_own, st_tot, st_max, probs, dprobs,
    acc_o, acc_dq, acc_dk, acc_dv, staged,
    in_loc, in_snd, in_rcv, seg_sem,
    r_snd, r_rcv, e_snd, e_rcv, l_snd, l_rcv, ready,
    out_snd, out_rcv,
):
    tok, feature = q_h.shape
    heads = HEADS // 2
    hd = feature // HEADS
    own = 2 * tok
    span = own - hd
    scale = math.log2(math.e) / math.sqrt(hd)
    inv_root = 1.0 / math.sqrt(hd)
    wide = 2 * hd

    def col(h, count=1):
        start = h * hd if isinstance(h, int) else pl.multiple_of(h * hd, hd)
        return pl.ds(start, count * hd)

    me = lax.axis_index("seq")
    core = lax.rem(me, 2)
    partner = me + 1 - 2 * core
    chip = lax.div(me, 2)
    left = lax.rem(me + n - 2, n)
    right = lax.rem(me + 2, n)
    has_left = chip > 0
    has_right = chip < n // 2 - 1

    barrier = pltpu.get_barrier_semaphore()

    def signal(sem, peer):
        pl.semaphore_signal(sem, inc=1, device_id={"seq": peer}, device_id_type=MESH)

    @pl.when(has_left)
    def _():
        for c in range(2):
            signal(barrier, 2 * lax.div(left, 2) + c)

    @pl.when((core == 1) | jnp.logical_not(has_right))
    def _():
        signal(barrier, partner)

    def remote(src, dst, snd, rcv, peer):
        return pltpu.make_async_remote_copy(
            src_ref=src, dst_ref=dst, send_sem=snd, recv_sem=rcv,
            device_id={"seq": peer}, device_id_type=MESH,
        )

    mine = pl.ds(pl.multiple_of(core * tok, tok), tok)
    theirs = pl.ds(pl.multiple_of((1 - core) * tok, tok), tok)
    pairs_in = ((k_h, k_all), (v_h, v_all), (q_h, q_all), (g_h, g_all))

    def group(which, s):
        return col(which * heads + s, 1 if s < DELAY else heads - DELAY)

    def in_local(j, s):
        src, dst = pairs_in[j]
        return pltpu.make_async_copy(src.at[:, group(core, s)], dst.at[mine, group(0, s)], in_loc.at[j, s])

    def in_remote(j, s):
        src, dst = pairs_in[j]
        return remote(
            src.at[:, group(1 - core, s)], dst.at[mine, group(0, s)], in_snd.at[j, s], in_rcv.at[j, s], partner
        )

    seg_local = pltpu.make_async_copy(seg_h, seg_buf.at[0, core], seg_sem.at[0])
    seg_remote = remote(seg_h, seg_buf.at[0, core], seg_sem.at[1], seg_sem.at[2], partner)

    def seg_right(source, target):
        return remote(
            seg_h, seg_buf.at[1, source], seg_sem.at[3 + target], seg_sem.at[7 + source],
            2 * lax.div(right, 2) + target,
        )

    seg_left = remote(seg_buf.at[0], seg_buf.at[2], seg_sem.at[5], seg_sem.at[6], left)
    pl.semaphore_wait(barrier, jnp.where(has_right, 3 - core, 1))

    @pl.when(has_right)
    def _():
        signal(ready.at[0], right)

    @pl.when(core == 0)
    def _():
        signal(ready.at[1], partner)

    head, below = pl.ds(0, span), pl.ds(2 * span, STAT)

    def early_left(t, i):
        src, dst = (
            (q_all.at[head, col(t)], rm.at[t, pl.ds(0, span)]),
            (g_all.at[head, col(t)], rm.at[t, pl.ds(span, span)]),
            (first.at[t], rm.at[t, below]),
        )[i]
        return remote(src, dst, e_snd.at[t, i], e_rcv.at[t, i], left)

    skip = own - span

    def early_right(t, i, source, target):
        count = tok - skip if source == 0 else tok
        at = i * span if source == 0 else i * span + tok - skip
        rows = pl.ds(skip, count) if source == 0 else pl.ds(0, count)
        return remote(
            pairs_in[i][0].at[rows, col(target * heads + t)], rp.at[t, pl.ds(at, count)],
            r_snd.at[t, i, target], r_rcv.at[t, i, source], 2 * lax.div(right, 2) + target,
        )

    def to_right(h):
        return remote(sendp.at[h], rp.at[h + DELAY], l_snd.at[0, h], l_rcv.at[0, h], right)

    def to_left(h):
        return remote(sendm.at[h], rm.at[h + DELAY], l_snd.at[1, h], l_rcv.at[1, h], left)

    for source in range(2):

        @pl.when(has_right & (core == source))
        def _():
            for target in range(2):
                seg_right(source, target).start()
            for t in range(DELAY):
                for target in range(2):
                    for i in range(2):
                        early_right(t, i, source, target).start()

    @pl.when(core == 1)
    def _():
        pl.semaphore_wait(ready.at[1], 1)

    seg_remote.start()
    seg_local.start()
    for s in range(DELAY + 1):
        for j in range(4):
            in_remote(j, s).start()
            in_local(j, s).start()

    @pl.when(jnp.logical_not(has_left))
    def _():
        seg_buf[1] = jnp.full(seg_buf.shape[1:], -1, jnp.int32)

        def clear(t, _):
            rp[t] = jnp.zeros(rp.shape[1:], BF16)
            return 0

        lax.fori_loop(0, rp.shape[0], clear, 0)

    @pl.when(jnp.logical_not(has_right))
    def _():
        seg_buf[2] = jnp.full(seg_buf.shape[1:], -3, jnp.int32)

        def clear(t, _):
            rm[t] = jnp.zeros(rm.shape[1:], BF16)
            return 0

        lax.fori_loop(0, rm.shape[0], clear, 0)

    seg_local.wait()
    seg_remote.wait_recv()

    def rows(ref, h, at, blocks):
        parts = [ref[h, at + b : at + b + 1, :] for b in range(blocks)]
        return parts[0] if blocks == 1 else jnp.concatenate(parts, axis=1)

    def put_rows(ref, h, at, value):
        for b in range(value.shape[1] // hd):
            ref[h, at + b : at + b + 1, :] = value[:, b * hd : (b + 1) * hd]

    def encode(lse, delta):
        out = []
        for row in lse:
            top = row.astype(BF16).astype(F32)
            mid = (row - top).astype(BF16).astype(F32)
            out += [top, mid, row - top - mid]
        for row in delta:
            top = row.astype(BF16).astype(F32)
            out += [top, row - top]
        out.append(jnp.zeros_like(out[0]))
        return jnp.concatenate(out, axis=0).astype(BF16)

    def decode(ref, t):
        table = ref[t, 2 * span : 2 * span + STAT, :].astype(F32)
        lse = [table[3 * b : 3 * b + 1] + table[3 * b + 1 : 3 * b + 2] + table[3 * b + 2 : 3 * b + 3] for b in range(3)]
        delta = [table[9 + 2 * b : 10 + 2 * b] + table[10 + 2 * b : 11 + 2 * b] for b in range(3)]
        return lse, delta

    def own_stats(h):
        lses, deltas = [], []
        for b in range(2):
            depth = (b + 1) * wide
            at = slice(b * wide, (b + 1) * wide)
            s = dot_nt(k_all[:depth, col(h)], q_all[at, col(h)]) * scale + b_own[:depth, at]
            dp = dot_nt(v_all[:depth, col(h)], g_all[at, col(h)])
            m = colmax(s)
            p = jnp.exp2(s - m)
            total = colsum(p)
            kept = slice(b * wide, b * wide + depth)
            probs[h, kept], dprobs[h, kept] = p, dp
            put_rows(st_max, h, 2 * b, m)
            lse, delta = m + jnp.log2(total), colsum(p * dp) / total
            put_rows(st_own, h, 2 * b, lse)
            put_rows(st_own, h, 4 + 2 * b, delta)
            lses += [lse[:, :hd], lse[:, hd:]]
            deltas += [delta[:, :hd], delta[:, hd:]]
        return encode(lses[:3], deltas[:3])

    def merge(lse, delta, parts):
        m = lse
        for s, _ in parts:
            m = jnp.maximum(m, colmax(s))
        first = jnp.exp2(lse - m)
        total, dn = first, delta * first
        probs = []
        for s, dp in parts:
            p = jnp.exp2(s - m)
            total = total + colsum(p)
            dn = dn + colsum(p * dp)
            probs.append(p)
        inv = 1.0 / total
        delta = dn * inv
        outs = []
        for p, (_, dp) in zip(probs, parts):
            p = p * inv
            outs.append((p.astype(BF16), (p * ((dp - delta) * inv_root)).astype(BF16)))
        return m + jnp.log2(total), delta, outs

    def cross(h):
        cut = span - wide
        nxt = jnp.minimum(h + DELAY, heads - 1)
        fresh = jnp.where(h + DELAY < heads, 1.0, 0.0)
        keys_right = jnp.broadcast_to((1.0 - flags[1:2, :]) * fresh, (span, hd)) > 0.5
        queries_left = jnp.broadcast_to(flags[0:1, :] * fresh, (span, hd)) > 0.5
        kl, vl = rp[h, :span], rp[h, span : 2 * span]
        lse_in, delta_in = decode(rm, h)
        k, v = k_all[:, col(h)], v_all[:, col(h)]
        qa, ga = rm[h, :wide], rm[h, span : span + wide]
        s1 = dot_nt(k, qa) * scale + b_right[:, :wide]
        s2 = dot_nt(kl[cut:], qa) * scale + b_far[...]
        d1, d2 = dot_nt(v, ga), dot_nt(vl[cut:], ga)
        lse, delta, ((p1, e1), (p2, e2)) = merge(
            jnp.concatenate(lse_in[:2], 1), jnp.concatenate(delta_in[:2], 1), ((s1, d1), (s2, d2))
        )
        lse_out, delta_out = [lse[:, :hd], lse[:, hd:]], [delta[:, :hd], delta[:, hd:]]
        @pl.when(has_left)
        def _():
            dkl_sum = dvl_sum = None
            dkl, dvl = dot_nn(e2, qa), dot_nn(p2, ga)
            stay_here = []
            for b in range(2):
                at = slice(b * wide, (b + 1) * wide)
                q, g = q_all[at, col(h)], g_all[at, col(h)]
                s = dot_nt(kl, q) * scale + b_left[:, at]
                dp = dot_nt(vl, g)
                lse, delta, ((p, e),) = merge(
                    rows(st_own, h, 2 * b, 2), rows(st_own, h, 4 + 2 * b, 2), ((s, dp),)
                )
                put_rows(st_tot, h, 2 * b, lse)
                put_rows(st_tot, h, 4 + 2 * b, delta)
                stay_here.append((at, p, e))
                dkb, dvb = dot_nn(e, q), dot_nn(p, g)
                dkl_sum = dkb if b == 0 else dkl_sum + dkb
                dvl_sum = dvb if b == 0 else dvl_sum + dvb
            for i, (total, extra, kept) in enumerate(((dkl_sum, dkl, q_all), (dvl_sum, dvl, g_all))):
                stay = kept[:span, col(nxt)].astype(F32)
                sendm[h, i * span : i * span + cut] = jnp.where(queries_left[:cut], stay[:cut], total[:cut]).astype(BF16)
                sendm[h, i * span + cut : (i + 1) * span] = jnp.where(
                    queries_left[cut:], stay[cut:], total[cut:] + extra
                ).astype(BF16)

            to_left(h).start()
            for at, p, e in stay_here:
                acc_o[h, at] = dot_tn(p, vl)
                acc_dq[h, at] = dot_tn(e, kl)

        for i, (a1, b1, a2, b2, kept) in enumerate(
            ((p1, v, p2, vl[cut:], k_all), (e1, k, e2, kl[cut:], v_all))
        ):
            part = dot_tn(a1, b1) + dot_tn(a2, b2)
            stay = kept[own - span : own - span + wide, col(nxt)].astype(F32)
            sendp[h, i * span : i * span + wide] = jnp.where(keys_right[:wide], stay, part).astype(BF16)
        qb, gb = rm[h, wide:span], rm[h, span + wide : 2 * span]
        s3 = dot_nt(k, qb) * scale + b_right[:, wide:]
        d3 = dot_nt(v, gb)
        lse, delta, ((p3, e3),) = merge(lse_in[2], delta_in[2], ((s3, d3),))
        sendp[h, 2 * span :] = encode(lse_out + [lse], delta_out + [delta])
        for i, (a3, b3, kept) in enumerate(((p3, v, k_all), (e3, k, v_all))):
            part = dot_tn(a3, b3)
            stay = kept[own - span + wide :, col(nxt)].astype(F32)
            sendp[h, i * span + wide : (i + 1) * span] = jnp.where(keys_right[wide:], stay, part).astype(BF16)

        @pl.when(has_right)
        def _():
            to_right(h).start()

        @pl.when(jnp.logical_not(has_left))
        def _():
            st_tot[h] = st_own[h]
            acc_o[h] = jnp.zeros((own, hd), F32)
            acc_dq[h] = jnp.zeros((own, hd), F32)

        acc_dk[h] = dot_nn(e1, qa) + dot_nn(e3, qb)
        acc_dv[h] = dot_nn(p1, ga) + dot_nn(p3, gb)

    def close(h):
        t = h + DELAY
        asked = flags[0:1, :] > 0.5
        back = jnp.broadcast_to(flags[0:1, :], (span, hd)) > 0.5
        back_keys = jnp.broadcast_to(1.0 - flags[1:2, :], (span, hd)) > 0.5
        lse = [st_tot[h, b : b + 1, :] for b in range(4)]
        delta = [st_tot[h, 4 + b : 5 + b, :] for b in range(4)]
        lse_back, delta_back = decode(rp, t)
        for b in range(3):
            lse[b] = jnp.where(asked, lse_back[b], lse[b])
            delta[b] = jnp.where(asked, delta_back[b], delta[b])
        add = [jnp.where(back, rp[t, i * span : (i + 1) * span].astype(F32), 0.0) for i in range(2)]
        for b in range(2):
            depth = (b + 1) * wide
            at = slice(b * wide, (b + 1) * wide)
            q, g = q_all[at, col(h)], g_all[at, col(h)]
            k, v = k_all[:depth, col(h)], v_all[:depth, col(h)]
            kept = slice(b * wide, b * wide + depth)
            shrink = jnp.exp2(rows(st_max, h, 2 * b, 2) - jnp.concatenate(lse[2 * b : 2 * b + 2], 1))
            p = probs[h, kept] * shrink
            e = (p * ((dprobs[h, kept] - jnp.concatenate(delta[2 * b : 2 * b + 2], 1)) * inv_root)).astype(BF16)
            p = p.astype(BF16)
            acc_dk[h, :depth] += dot_nn(e, q)
            acc_dv[h, :depth] += dot_nn(p, g)
            for i, (value, acc) in enumerate(((dot_tn(p, v), acc_o), (dot_tn(e, k), acc_dq))):
                value = value + acc[h, at]
                if b == 0:
                    staged[h, i, at] = (value + add[i][:wide]).astype(BF16)
                else:
                    staged[h, i, wide:span] = (value[: span - wide] + add[i][wide:]).astype(BF16)
                    staged[h, i, span:] = value[span - wide :].astype(BF16)
        for j in range(2):
            out_remote(j, h).start()
        for i, acc in ((0, acc_dk), (1, acc_dv)):
            staged[h, 2 + i, : own - span] = acc[h, : own - span].astype(BF16)
            staged[h, 2 + i, own - span :] = (
                acc[h, own - span :] + jnp.where(back_keys, rm[t, i * span : (i + 1) * span].astype(F32), 0.0)
            ).astype(BF16)

    outs = (o_h, dq_h, dk_h, dv_h)

    def out_remote(j, h):
        return remote(
            staged.at[h, j, theirs], outs[j].at[:, col(core * heads + h)],
            out_snd.at[j, h], out_rcv.at[j, h], partner,
        )

    def seg_row(chip, b):
        return seg_buf[chip, b // 2, b % 2 : b % 2 + 1, :].astype(F32)

    def as_column(row):
        return jnp.transpose(jnp.broadcast_to(row, (hd, hd)))

    def tile(a, b):
        return slice(a * hd, (a + 1) * hd), slice(b * hd, (b + 1) * hd)

    own_rows = [seg_row(0, b) for b in range(4)]
    own_cols = [as_column(row) for row in own_rows]
    causal = lax.broadcasted_iota(jnp.int32, (hd, hd), 0) <= lax.broadcasted_iota(jnp.int32, (hd, hd), 1)
    for a in range(4):
        for b in range(4):
            same = own_cols[a] == own_rows[b]
            if a > b:
                b_own[tile(a, b)] = jnp.full((hd, hd), NEG, F32)
            else:
                b_own[tile(a, b)] = jnp.where(same & causal if a == b else same, 0.0, NEG)

    for t in range(DELAY):
        for j in range(4):
            in_local(j, t).wait()
            in_remote(j, t).wait_recv()
        if t == 0:
            first[0] = own_stats(0)
        else:

            @pl.when(has_left)
            def _():
                first[t] = own_stats(t)

    @pl.when(has_left)
    def _():
        pl.semaphore_wait(ready.at[0], 1)
        seg_left.start()
        for t in range(DELAY):
            for i in range(3):
                early_left(t, i).start()
        for source in range(2):
            seg_right(source, 0).wait_recv()

    @pl.when(has_right)
    def _():
        seg_left.wait_recv()

    def seg_at(chip, b, lane):
        return jnp.broadcast_to(seg_row(chip, b)[:, lane : lane + 1], (1, hd))

    asks_left = seg_at(1, 0, hd - 1) == seg_at(0, 0, 0)
    asks_right = seg_at(0, 0, hd - 1) == seg_at(2, 0, 0)
    flags[0:1, :] = jnp.where(asks_left, 1.0, 0.0)
    flags[1:2, :] = jnp.where(asks_right, 1.0, 0.0)
    left_cols = [as_column(jnp.where(asks_left, -1.0, seg_row(1, b + 1))) for b in range(3)]
    right_rows = [jnp.where(asks_right, seg_row(2, b), -2.0) for b in range(3)]
    for a in range(4):
        for b in range(4):
            if a < 3:
                b_left[tile(a, b)] = jnp.where(left_cols[a] == own_rows[b], 0.0, NEG)
            if b < 3:
                b_right[tile(a, b)] = jnp.where(own_cols[a] == right_rows[b], 0.0, NEG)
            if a < 2 and b < 2:
                b_far[tile(a, b)] = jnp.where(left_cols[a + 1] == right_rows[b], 0.0, NEG)

    def step(i, _):
        @pl.when(i == 0)
        def _():
            for j in range(4):
                in_local(j, DELAY).wait()
                in_remote(j, DELAY).wait_recv()

        @pl.when((i + DELAY < heads) & has_left)
        def _():
            sendm[i, 2 * span :] = own_stats(i + DELAY)

        @pl.when(i >= heads - DELAY)
        def _():
            @pl.when(i < heads)
            def _():
                sendm[i, 2 * span :] = jnp.zeros((STAT, hd), BF16)

        @pl.when((i < DELAY) & has_left)
        def _():
            for j in range(2):
                for source in range(2):
                    early_right(i, j, source, 0).wait_recv()
            for j in range(3):
                early_left(i, j).wait_send()

        @pl.when((i < DELAY) & has_right)
        def _():
            for j in range(3):
                early_left(i, j).wait_recv()

        @pl.when((i >= DELAY) & has_left)
        def _():
            to_right(i - DELAY).wait_recv()
            to_left(i - DELAY).wait_send()

        @pl.when((i >= DELAY) & has_right)
        def _():
            to_left(i - DELAY).wait_recv()
            to_right(i - DELAY).wait_send()

        @pl.when(i < heads)
        def _():
            cross(i)

        @pl.when((i < heads - 1) & jnp.logical_not(has_left))
        def _():
            own_stats(i + 1)

        @pl.when(i >= DELAY)
        def _():
            h = i - DELAY
            close(h)
            for j in range(2, 4):
                out_remote(j, h).start()
            for j in range(4):
                outs[j][:, col(core * heads + h)] = staged[h, j, mine, :]

        @pl.when(i > DELAY)
        def _():
            for j in range(4):
                out_remote(j, i - DELAY - 1).wait()

        return 0

    lax.fori_loop(0, heads + DELAY, step, 0)
    for s in range(DELAY + 1):
        for j in range(4):
            in_remote(j, s).wait_send()
    for j in range(4):
        out_remote(j, heads - 1).wait()
    seg_remote.wait_send()

    for source in range(2):

        @pl.when(has_right & (core == source))
        def _():
            for t in range(DELAY):
                for target in range(2):
                    for i in range(2):
                        early_right(t, i, source, target).wait_send()

    @pl.when(has_right)
    def _():
        for target in range(2):
            seg_right(0, target).wait_send()

    @pl.when(has_left)
    def _():
        seg_left.wait_send()


def store(*refs):
    sem = refs[8]
    copies = [pltpu.make_async_copy(refs[j], refs[4 + j], sem.at[j]) for j in range(4)]
    for copy in copies:
        copy.start()
    for copy in copies:
        copy.wait()


def local(n, queries, keys, values, out_grad, segments):
    tok, feature = queries.shape
    heads, hd = HEADS // 2, feature // HEADS
    own = 2 * tok
    span = own - hd
    slots = heads + DELAY
    rows = 2 * span + STAT
    out = jax.ShapeDtypeStruct((tok, feature), BF16)
    dma = pltpu.SemaphoreType.DMA
    vm = pltpu.VMEM
    results = pl.pallas_call(
        functools.partial(kernel, n),
        out_shape=(vm((tok, feature), BF16),) * 4,
        in_specs=[pl.BlockSpec(memory_space=pltpu.HBM)] * 5,
        out_specs=[pl.BlockSpec(memory_space=vm)] * 4,
        scratch_shapes=[
            vm((own, heads * hd), BF16), vm((own, heads * hd), BF16),
            vm((own, heads * hd), BF16), vm((own, heads * hd), BF16),
            vm((3, 2, 2, hd), jnp.int32), vm((8, hd), F32),
            vm((own, own), F32), vm((span, own), F32), vm((own, span), F32), vm((2 * hd, 2 * hd), F32),
            vm((slots, rows, hd), BF16), vm((slots, rows, hd), BF16),
            vm((heads, rows, hd), BF16), vm((heads, rows, hd), BF16), vm((DELAY, STAT, hd), BF16),
            vm((heads, 8, hd), F32), vm((heads, 8, hd), F32), vm((heads, 8, hd), F32),
            vm((heads, 6 * hd, 2 * hd), F32), vm((heads, 6 * hd, 2 * hd), F32),
            vm((heads, own, hd), F32), vm((heads, own, hd), F32),
            vm((heads, own, hd), F32), vm((heads, own, hd), F32),
            vm((heads, 4, own, hd), BF16),
            dma((4, DELAY + 1)), dma((4, DELAY + 1)), dma((4, DELAY + 1)), dma((9,)),
            dma((DELAY, 2, 2)), dma((DELAY, 2, 2)), dma((DELAY, 3)), dma((DELAY, 3)),
            dma((2, heads)), dma((2, heads)), pltpu.SemaphoreType.REGULAR((2,)),
            dma((4, heads)), dma((4, heads)),
        ],
        compiler_params=pltpu.CompilerParams(
            collective_id=0, has_side_effects=True, vmem_limit_bytes=51 * 2**20
        ),
        name="packed_attention",
    )(*(pltpu.with_memory_space_constraint(x, pltpu.HBM) for x in (queries, keys, values, out_grad)), segments.reshape(2, tok // 2))
    return pl.pallas_call(
        store,
        out_shape=(out,) * 4,
        in_specs=[pl.BlockSpec(memory_space=pl.ANY)] * 4,
        out_specs=[pl.BlockSpec(memory_space=pl.ANY)] * 4,
        scratch_shapes=[dma((4,))],
        compiler_params=pltpu.CompilerParams(vmem_limit_bytes=2**20),
        name="store_results",
    )(*(pltpu.with_memory_space_constraint(r, vm) for r in results))


def solution(mesh):
    spec = P(("branch", "seq"), None)
    return jax.shard_map(
        functools.partial(local, mesh.shape["seq"]),
        mesh=mesh,
        in_specs=(spec,) * 4 + (P(("branch", "seq")),),
        out_specs=(spec,) * 4,
        check_vma=False,
    )
```
